32 devices in a mesh: groups: 2 (over x), blk: 16 (over z, y, core).
Axes of the slice: x: 2, y: 2, z: 4, core: 2. Of those that a mesh axis runs over, the one named last changes fastest.
Arguments:
- pair_elements: float32 [12288, 1024], P(('groups', 'blk')), parts along dimension 0, may hold values from -0.8 to 0.8
- gmap: int32 [12288], P(('groups', 'blk')), parts along dimension 0, may hold values from 0 to 6143, as said below
- w_screened: float32 [12288, 6144], P('groups', 'blk'), parts along dimension 0, as said below
- coulomb: float32 [12288], P(('groups', 'blk')), parts along dimension 0, may hold values from 0.001 to 0.02
Outputs:
- screened: float32 [12288, 1024], P(('groups', 'blk')), parts along dimension 0
- pair_sigma: float32 [2048], P(('groups', 'blk')), parts along dimension 0
The draws below stay inside these ranges and needn't reach their ends.
There are 2 independent parts, one for each index of `groups`. The reference program is written for one: setup_inputs(seed, part) draws one part's arguments, and reference() takes and returns one part's arrays. A program takes and returns all parts, laid end to end along the dimension named above; each array names one. Nothing has to cross between parts.
Inputs may be any that keep to these rules, and one draw needn't show every extreme that they name: `gmap`: each aligned block of 384 entries is a permutation of that block's own indices. `w_screened`: symmetric.
All inputs are finite; a program needn't handle non-finite values.
Results may differ from the reference program's by a relative error of at most 0.00013.
Values sent between devices are 32-bit elements; how exact they have to be, the bound alone decides.
No kernel may reach another device: no remote copies, remote signals or barrier semaphores. Data moves between devices by JAX's collectives and lax.ppermute only.
A program may use at most 256 MiB of HBM per device.

```python
import math
import jax
import jax.numpy as jnp
from jax import lax

G_DEV = 384
NG = 6144
NB = 64
OCC = 4
P_SIZE = 1024


def draw_gmap(key, part):
    blocks = NG // G_DEV
    scores = jax.random.randint(key, (blocks, G_DEV), 0, 1 << 30)
    scores = scores * G_DEV + jnp.arange(G_DEV, dtype=jnp.int32)[None, :]
    order = jnp.argsort(scores, axis=1, stable=True).astype(jnp.int32)
    offsets = (jnp.arange(blocks, dtype=jnp.int32) * G_DEV)[:, None]
    return (order + offsets).reshape(NG).astype(jnp.int32)


def draw_w_screened(key, part):
    base = jax.random.normal(key, (NG, NG), jnp.float32)
    return ((base + base.T) * (0.5 / NG) ** 0.5).astype(jnp.float32)


def raised(entries, own_key, source, target, shards_of, factor):
    def block_of(dim):
        return (jnp.arange(entries.shape[dim]) // (entries.shape[dim] // shards_of)).reshape((-1,) + (1,) * (entries.ndim - 1 - dim))

    first = jax.random.permutation(own_key, shards_of)[block_of(target)]
    far = (block_of(target) + shards_of // 2) % shards_of
    return jnp.where((block_of(source) == first) | (block_of(source) == far), factor * entries, entries)


def steps_of(key, dims, shards, smallest, top_value):
    level, own = 1.0, jax.random.fold_in(key, 6)
    for axis_at, shards_of in shards:
        steps = jnp.exp(jax.random.uniform(jax.random.fold_in(own, axis_at), (shards_of,), jnp.float32, smallest / len(shards), top_value / len(shards)))
        level = level * jnp.repeat(steps, dims[axis_at] // shards_of).reshape([-1 if axis == axis_at else 1 for axis in range(len(dims))])
    return level


def noise_with(own_key, dims, deviation, reach, cuts, heavy, kind=jnp.bfloat16):
    result = deviation * jax.random.normal(own_key, dims, jnp.float32)
    if cuts:
        result = result * steps_of(own_key, dims, cuts, -0.22, 0.18)
    return jnp.clip(raised(result, jax.random.fold_in(own_key, 3), *heavy), -reach, reach).astype(kind)


def setup_inputs(seed: int = 0, part: int = 0) -> dict:
    key_list = jax.random.split(jax.random.key(seed), 5)
    part_keys = jax.random.split(jax.random.fold_in(key_list[4], part), 5)
    return {
        "pair_elements": noise_with(part_keys[0], (NG, P_SIZE), 0.1, 0.8, ((0, 16),), (0, 1, 16, 2.0), jnp.float32),
        "gmap": draw_gmap(jax.random.fold_in(jax.random.fold_in(key_list[4], part), 71), part),
        "w_screened": draw_w_screened(jax.random.fold_in(jax.random.fold_in(key_list[4], part), 71), part),
        "coulomb": jnp.clip(jnp.exp(math.log(0.02) - 2.9957322 * jax.random.uniform(part_keys[3], (NG,), jnp.float32) ** steps_of(part_keys[3], (NG,), ((0, 16),), -0.2, 0.2)), 0.001, 0.02),
    }


def reference(pair_elements, gmap, w_screened, coulomb):
    elements = jnp.take(pair_elements, gmap.astype(jnp.int32), axis=0)
    screened = lax.dot_general(w_screened, elements, (((0,), (0,)), ((), ())), precision=lax.Precision.HIGHEST, preferred_element_type=jnp.float32)
    band = jnp.arange(P_SIZE, dtype=jnp.int32) % NB
    coef = jnp.where(band < OCC, -0.5, 0.5).astype(jnp.float32)
    pair_sigma = coef * jnp.sum(screened * elements, axis=0) - 0.5 * jnp.sum(coulomb[:, None] * elements * elements, axis=0)
    return screened, pair_sigma
```

```python
import jax
import jax.numpy as jnp
from jax import lax
from jax.sharding import PartitionSpec as P

NB = 64
OCC = 4
CHAINS = 4


def chip_ring(mesh):
    row = mesh.devices.reshape(mesh.shape["groups"], -1)[0]
    places = [tuple(getattr(d, "coords", (0, 0, i // 2))) for i, d in enumerate(row)]
    chips = {}
    for index, place in enumerate(places):
        chips.setdefault(place, []).append(index)
    ordered = []
    spread = [len({p[k] for p in chips}) for k in range(3)]
    long = max(range(3), key=lambda k: spread[k])
    lanes = {}
    for p in chips:
        lanes.setdefault(tuple(v for k, v in enumerate(p) if k != long), []).append(p)
    for number, lane in enumerate(sorted(lanes)):
        line = sorted(lanes[lane], key=lambda p: p[long])
        ordered += line[::-1] if number % 2 else line
    return [chips[p] for p in ordered]


def solution(mesh):
    ring = chip_ring(mesh)
    n = len(ring)
    cores = len(ring[0])
    ahead = [(a, b) for i in range(n) for a, b in zip(ring[i], ring[(i + 1) % n])]
    back = [(b, a) for a, b in ahead]
    partner = [(chip[c], chip[(c + 1) % cores]) for chip in ring for c in range(cores)]
    size = n * cores
    place = [0] * size
    for i, chip in enumerate(ring):
        for index in chip:
            place[index] = i

    def local(pair_elements, gmap, w_screened, coulomb):
        rows = pair_elements.shape[0]
        width = pair_elements.shape[1]
        me = lax.axis_index("blk")
        spot = jnp.array(place, jnp.int32)[me]
        core = jnp.array([chip.index(i) for i in range(size) for chip in ring if i in chip], jnp.int32)[me]
        order = jnp.array(ring, jnp.int32)
        elements = pair_elements.at[gmap % rows].get(mode="promise_in_bounds")

        def dot(block, x):
            w = lax.dynamic_slice(w_screened, (block * rows, 0), (rows, rows))
            return lax.dot_general(
                w, x, (((0,), (0,)), ((), ())), precision=lax.Precision.HIGH, preferred_element_type=jnp.float32
            )

        band = jnp.arange(width, dtype=jnp.int32) % NB
        coef = jnp.where(band < OCC, -0.5, 0.5).astype(jnp.float32)
        bare = jnp.sum(coulomb[:, None] * elements * elements, axis=0)
        quarter = width // CHAINS
        held = [elements[:, j * quarter : (j + 1) * quarter] for j in range(CHAINS)]
        mine = list(held)
        total = [None] * CHAINS
        form = [None] * CHAINS
        for step in range(n):
            for j in range(CHAINS):
                if step:
                    held[j] = lax.ppermute(held[j], "blk", back if j % 2 else ahead)
                other = lax.ppermute(held[j], "blk", partner)
                source = (spot + (step if j % 2 else n - step)) % n
                part = dot(order[source, core], held[j]) + dot(order[source, (core + cores - 1) % cores], other)
                total[j] = part if step == 0 else total[j] + part
                if step in (0, n // 2 - 1, n // 2):
                    s = jnp.sum(total[j] * mine[j], axis=0)
                    form[j] = -s if step == 0 else form[j] + s
            if step == n // 2:
                terms = coef * jnp.concatenate(form) - 0.5 * bare
                k = size // 2
                while k:
                    bit = (me // k) % 2
                    terms = terms.reshape(2, -1)
                    keep = jnp.where(bit == 0, terms[0], terms[1])
                    send = jnp.where(bit == 0, terms[1], terms[0])
                    terms = keep + lax.ppermute(send, "blk", [(b, b ^ k) for b in range(size)])
                    k //= 2
        return jnp.concatenate(total, axis=1), terms

    in_specs = (
        P(("groups", "blk"), None),
        P(("groups", "blk")),
        P("groups", "blk"),
        P(("groups", "blk")),
    )
    out_specs = (P(("groups", "blk"), None), P(("groups", "blk")))
    return jax.shard_map(local, mesh=mesh, in_specs=in_specs, out_specs=out_specs, check_vma=False)
```

```python
import functools

import jax
import jax.numpy as jnp
from jax import lax
from jax.experimental import pallas as pl
from jax.experimental.pallas import tpu as pltpu
from jax.sharding import PartitionSpec as P


NB = 64
OCC = 4
LIMIT = 20 << 20
DOTS_LIMIT = 46 << 20


def chip_ring(mesh):
    row = mesh.devices.reshape(mesh.shape["groups"], -1)[0]
    places = [tuple(getattr(d, "coords", (0, 0, i // 2))) for i, d in enumerate(row)]
    chips = {}
    for index, place in enumerate(places):
        chips.setdefault(place, []).append(index)
    ordered = []
    spread = [len({p[k] for p in chips}) for k in range(3)]
    long = max(range(3), key=lambda k: spread[k])
    lanes = {}
    for p in chips:
        lanes.setdefault(tuple(v for k, v in enumerate(p) if k != long), []).append(p)
    for number, lane in enumerate(sorted(lanes)):
        line = sorted(lanes[lane], key=lambda p: p[long])
        ordered += line[::-1] if number % 2 else line
    return [chips[p] for p in ordered]


def split(x):
    high = x.astype(jnp.bfloat16)
    return high, (x - high.astype(jnp.float32)).astype(jnp.bfloat16)


def dots_kernel(at, first, watch, blocks, x0, x1, w_own, w_partner, *refs):
    landed, sems = refs[-2:]
    refs = refs[:-2]
    rows = landed.shape[1]
    wide = x0.shape[0]
    copies = []
    for way in (0, 1):
        here = pl.ds(pl.multiple_of(blocks[at + way] * rows, rows), rows)
        for k, w in enumerate((w_own, w_partner)):
            copies.append(pltpu.make_async_copy(w.at[here], landed.at[2 * way + k], sems.at[2 * way + k]))
    for copy in copies:
        copy.start()
    for way, x in enumerate((x0, x1)):
        mine = pl.ds(way * wide, wide)
        xh, xl = split(x[...])
        left = jnp.concatenate([xh, xl, xh], 1)
        for k in (0, 1):
            copies[2 * way + k].wait()
            wh, wl = split(landed[2 * way + k])
            lanes = pl.ds(k * rows, rows)
            total = jnp.dot(left, jnp.concatenate([wh, wh, wl], 0), preferred_element_type=jnp.float32)
            if not first:
                total = refs[0][mine, lanes] + total
            refs[-watch - 1][mine, lanes] = total
            if watch:
                product = total * refs[1 + way + 2 * k][...]
                seen = functools.reduce(lambda p, q: p + q, [product[:, i : i + 128] for i in range(0, rows, 128)])
                refs[-1][mine, :] = seen if k == 0 else refs[-1][mine, :] + seen


def dots(blocks, at, pieces, w_own, w_partner, total=None, start=None):
    wide, rows = pieces[0].shape
    vmem = pl.BlockSpec(memory_space=pltpu.VMEM)
    hbm = pl.BlockSpec(memory_space=pltpu.HBM)
    more = [] if total is None else [total]
    watch = [] if start is None else list(start)
    shape = jax.ShapeDtypeStruct((2 * wide, 2 * rows), jnp.float32)
    form = jax.ShapeDtypeStruct((2 * wide, 128), jnp.float32)
    out = pl.pallas_call(
        functools.partial(dots_kernel, at, total is None, int(start is not None)),
        out_shape=(shape, form) if watch else (shape,),
        in_specs=[pl.BlockSpec(memory_space=pltpu.SMEM), vmem, vmem, hbm, hbm] + [vmem] * (len(more) + len(watch)),
        out_specs=(vmem, vmem)[: 2 if watch else 1],
        scratch_shapes=[pltpu.VMEM((4, rows, rows), jnp.float32), pltpu.SemaphoreType.DMA((4,))],
        input_output_aliases={5: 0} if more else {},
        cost_estimate=pl.CostEstimate(
            flops=24 * rows * rows * wide, bytes_accessed=16 * rows * rows, transcendentals=0
        ),
        compiler_params=pltpu.CompilerParams(vmem_limit_bytes=DOTS_LIMIT),
        name="dots",
    )(blocks, *pieces, w_own, w_partner, *more, *watch)
    return out if watch else (out[0], None)


def take_kernel(core, block, gmap, *outs):
    rows, width = block.shape
    quarter = width // 4
    pick = (lax.broadcasted_iota(jnp.int32, (rows, rows), 0) == gmap[...]).astype(jnp.bfloat16)
    pick = jnp.concatenate([pick, pick, pick], 0)
    for at in range(4):
        col = jnp.where(core[0] == 0, at, (at + 2) % 4) * quarter
        x = block[:, pl.ds(pl.multiple_of(col, quarter), quarter)].T
        high, rest = split(x)
        rest = x - high.astype(jnp.float32)
        mid, low = split(rest)
        got = jnp.dot(jnp.concatenate([high, mid, low], 1), pick, preferred_element_type=jnp.float32)
        if at < 2:
            outs[at][...] = got
        else:
            outs[2][(at - 2) * quarter : (at - 1) * quarter, :] = got


def take(core, pair_elements, local_rows):
    rows, width = pair_elements.shape
    piece = jax.ShapeDtypeStruct((width // 4, rows), jnp.float32)
    return pl.pallas_call(
        take_kernel,
        out_shape=(piece, piece, jax.ShapeDtypeStruct((width // 2, rows), jnp.float32)),
        in_specs=[
            pl.BlockSpec(memory_space=pltpu.SMEM),
            pl.BlockSpec(memory_space=pltpu.VMEM),
            pl.BlockSpec(memory_space=pltpu.VMEM),
        ],
        out_specs=[pl.BlockSpec(memory_space=pltpu.VMEM)] * 3,
        cost_estimate=pl.CostEstimate(flops=6 * rows * rows * width, bytes_accessed=8 * rows * width, transcendentals=0),
        compiler_params=pltpu.CompilerParams(vmem_limit_bytes=LIMIT),
        name="take",
    )(core.reshape(1), pair_elements, local_rows.reshape(1, rows))


def turn_kernel(core, x, *refs):
    refs[-1][...] = x[...].T


def turn(at, x, rows, out=None):
    half = x.shape[0]
    more = [] if out is None else [out]
    return pl.pallas_call(
        turn_kernel,
        out_shape=jax.ShapeDtypeStruct((rows, 2 * half), jnp.float32),
        grid_spec=pltpu.PrefetchScalarGridSpec(
            num_scalar_prefetch=1,
            grid=(2,),
            in_specs=[pl.BlockSpec((half // 2, rows), lambda i, c: (i, 0))]
            + [pl.BlockSpec(memory_space=pl.ANY)] * len(more),
            out_specs=pl.BlockSpec((rows, half // 2), lambda i, c: (0, 2 * c[0] + i)),
        ),
        input_output_aliases={2: 0} if more else {},
        compiler_params=pltpu.CompilerParams(vmem_limit_bytes=LIMIT),
        name="turn",
    )(at.reshape(1), x, *more)


def solution(mesh):
    ring = chip_ring(mesh)
    n = len(ring)
    size = 2 * n
    ahead = [(a, b) for i in range(n) for a, b in zip(ring[i], ring[(i + 1) % n])]
    back = [(b, a) for a, b in ahead]
    partner = [(i, i ^ 1) for i in range(size)]
    spot_of = {index: i for i, chip in enumerate(ring) for index in chip}
    sources = [
        [[ring[(spot_of[d] - step * way) % n][0] // 2 for step in range(n)] for way in (1, -1)] for d in range(size)
    ]

    def local(pair_elements, gmap, w_screened, coulomb):
        rows, width = pair_elements.shape
        half = width // 2
        wide = half // 2
        me = lax.axis_index("blk")
        core = me % 2
        source = lax.dynamic_index_in_dim(jnp.array(sources, jnp.int32), me, 0, keepdims=False)
        blocks = (2 * source.T[:, None, :] + ((core + jnp.arange(2)) % 2)[None, :, None]).reshape(n * 4)
        here = core * half
        w_partner = lax.ppermute(w_screened, "blk", partner)
        *mine, away = take(core, pair_elements, lax.rem(gmap, rows))
        given = lax.ppermute(away, "blk", partner)
        held = [mine, [given[way * wide : (way + 1) * wide] for way in (0, 1)]]
        start = list(held)

        band = (here + jnp.arange(half, dtype=jnp.int32)) % NB
        coef = jnp.where(band < OCC, -0.5, 0.5).astype(jnp.float32)
        start = [x for pair in start for x in pair]
        total = None
        form = None
        terms = None
        bit_at = size // 2

        def exchange(terms, bit_at):
            bit = (me // bit_at) % 2
            terms = terms.reshape(2, -1)
            keep = jnp.where(bit == 0, terms[0], terms[1])
            send = jnp.where(bit == 0, terms[1], terms[0])
            return keep + lax.ppermute(send, "blk", [(b, b ^ bit_at) for b in range(size)])

        for step in range(n):
            for c in (0, 1):
                if step:
                    held[c] = [lax.ppermute(held[c][way], "blk", back if way else ahead) for way in (0, 1)]
                look = c == 1 and step in (0, n // 2 - 1, n // 2)
                total, seen = dots(
                    blocks, 4 * step + 2 * c, held[c], w_screened, w_partner, total, start if look else None
                )
                if look:
                    form = -seen if step == 0 else form + seen
            if step == n // 2:
                own_bare = -0.5 * jnp.sum(jnp.concatenate(mine, 0) ** 2 * coulomb[None, :], axis=1)
                away_bare = -0.5 * jnp.sum(away * away * coulomb[None, :], axis=1)
                form = own_bare + coef * jnp.sum(form, axis=1)
                terms = jnp.where(core == 0, jnp.concatenate([form, away_bare]), jnp.concatenate([away_bare, form]))
            elif terms is not None and bit_at:
                terms = exchange(terms, bit_at)
                bit_at //= 2
        while bit_at:
            terms = exchange(terms, bit_at)
            bit_at //= 2
        other = lax.ppermute(total[:, rows:], "blk", partner)
        screened = turn(1 - core, other, rows, turn(core, total, rows))
        return screened, terms

    in_specs = (
        P(("groups", "blk"), None),
        P(("groups", "blk")),
        P("groups", "blk"),
        P(("groups", "blk")),
    )
    out_specs = (P(("groups", "blk"), None), P(("groups", "blk")))
    return jax.shard_map(local, mesh=mesh, in_specs=in_specs, out_specs=out_specs, check_vma=False)
```

```python
import functools

import jax
import jax.numpy as jnp
from jax import lax
from jax.experimental import pallas as pl
from jax.experimental.pallas import tpu as pltpu
from jax.sharding import PartitionSpec as P


NB = 64
OCC = 4
LIMIT = 20 << 20
DOTS_LIMIT = 46 << 20


def chip_ring(mesh):
    row = mesh.devices.reshape(mesh.shape["groups"], -1)[0]
    places = [tuple(getattr(d, "coords", (0, 0, i // 2))) for i, d in enumerate(row)]
    chips = {}
    for index, place in enumerate(places):
        chips.setdefault(place, []).append(index)
    ordered = []
    spread = [len({p[k] for p in chips}) for k in range(3)]
    long = max(range(3), key=lambda k: spread[k])
    lanes = {}
    for p in chips:
        lanes.setdefault(tuple(v for k, v in enumerate(p) if k != long), []).append(p)
    for number, lane in enumerate(sorted(lanes)):
        line = sorted(lanes[lane], key=lambda p: p[long])
        ordered += line[::-1] if number % 2 else line
    return [chips[p] for p in ordered]


def split(x):
    high = x.astype(jnp.bfloat16)
    return high, (x - high.astype(jnp.float32)).astype(jnp.bfloat16)


def dots_kernel(at, first, watch, blocks, x0, x1, w_own, w_partner, *refs):
    left, landed, sems = refs[-3:]
    refs = refs[:-3]
    out = refs[-watch - 1]
    rows = landed.shape[1]
    wide = x0.shape[0]

    def copies(way):
        here = pl.ds(pl.multiple_of(blocks[at + way] * rows, rows), rows)
        for k, w in enumerate((w_own, w_partner)):
            yield pltpu.make_async_copy(
                w.at[here], landed.at[way, :, k * rows : (k + 1) * rows], sems.at[way, k]
            )

    for way in (0, 1):
        for copy in copies(way):
            copy.start()
    for way, x in enumerate((x0, x1)):
        xh, xl = split(x[...])
        for i, part in enumerate((xh, xl, xh)):
            left[way, :, i * rows : (i + 1) * rows] = part

    def product(way):
        for copy in copies(way):
            copy.wait()
        wh, wl = split(landed[way])
        total = jnp.dot(left[way], jnp.concatenate([wh, wh, wl], 0), preferred_element_type=jnp.float32)
        mine = pl.ds(way * wide if isinstance(way, int) else pl.multiple_of(way * wide, wide), wide)
        if not first:
            total = refs[0][mine, :] + total
        out[mine, :] = total
        return total

    if watch:
        for way in (0, 1):
            seen = product(way) * jnp.concatenate([refs[1 + way][...], refs[3 + way][...]], 1)
            seen = functools.reduce(lambda p, q: p + q, [seen[:, i : i + 128] for i in range(0, 2 * rows, 128)])
            refs[-1][way * wide : (way + 1) * wide, :] = seen
    else:

        @pl.loop(0, 2)
        def _(way):
            product(way)


def dots(blocks, at, pieces, w_own, w_partner, total=None, start=None):
    wide, rows = pieces[0].shape
    vmem = pl.BlockSpec(memory_space=pltpu.VMEM)
    hbm = pl.BlockSpec(memory_space=pltpu.HBM)
    more = [] if total is None else [total]
    watch = [] if start is None else list(start)
    shape = jax.ShapeDtypeStruct((2 * wide, 2 * rows), jnp.float32)
    form = jax.ShapeDtypeStruct((2 * wide, 128), jnp.float32)
    out = pl.pallas_call(
        functools.partial(dots_kernel, at, total is None, int(start is not None)),
        out_shape=(shape, form) if watch else (shape,),
        in_specs=[pl.BlockSpec(memory_space=pltpu.SMEM), vmem, vmem, hbm, hbm] + [vmem] * (len(more) + len(watch)),
        out_specs=(vmem, vmem)[: 2 if watch else 1],
        scratch_shapes=[
            pltpu.VMEM((2, wide, 3 * rows), jnp.bfloat16),
            pltpu.VMEM((2, rows, 2 * rows), jnp.float32),
            pltpu.SemaphoreType.DMA((2, 2)),
        ],
        input_output_aliases={5: 0} if more else {},
        cost_estimate=pl.CostEstimate(
            flops=24 * rows * rows * wide, bytes_accessed=16 * rows * rows, transcendentals=0
        ),
        compiler_params=pltpu.CompilerParams(vmem_limit_bytes=DOTS_LIMIT),
        name="dots",
    )(blocks, *pieces, w_own, w_partner, *more, *watch)
    return out if watch else (out[0], None)


def fetch_kernel(at, blocks, w_own, w_partner, out, landed, sems):
    rows = landed.shape[1]
    copies = []
    for k, w in enumerate((w_partner, w_own)):
        for way in (0, 1):
            here = pl.ds(pl.multiple_of(blocks[at + way] * rows, rows), rows)
            copies.append(pltpu.make_async_copy(w.at[here], landed.at[2 * k + way], sems.at[2 * k + way]))
    for copy in copies:
        copy.start()
    for i, copy in enumerate(copies):
        copy.wait()
        high, low = split(landed[i])
        out[i] = jnp.concatenate([high, high, low], 0)


def fetch(blocks, at, w_own, w_partner):
    rows = w_own.shape[1]
    hbm = pl.BlockSpec(memory_space=pltpu.HBM)
    return pl.pallas_call(
        functools.partial(fetch_kernel, at),
        out_shape=jax.ShapeDtypeStruct((4, 3 * rows, rows), jnp.bfloat16),
        in_specs=[pl.BlockSpec(memory_space=pltpu.SMEM), hbm, hbm],
        out_specs=pl.BlockSpec(memory_space=pltpu.VMEM),
        scratch_shapes=[pltpu.VMEM((4, rows, rows), jnp.float32), pltpu.SemaphoreType.DMA((4,))],
        cost_estimate=pl.CostEstimate(flops=8 * rows * rows, bytes_accessed=40 * rows * rows, transcendentals=0),
        compiler_params=pltpu.CompilerParams(vmem_limit_bytes=DOTS_LIMIT),
        name="fetch",
    )(blocks, w_own, w_partner)


def finish_kernel(k, x0, x1, right, total, out):
    wide, rows = x0.shape
    for way, x in enumerate((x0, x1)):
        mine = slice(way * wide, (way + 1) * wide)
        xh, xl = split(x[...])
        part = jnp.dot(
            jnp.concatenate([xh, xl, xh], 1), right[2 * (1 - k) + way], preferred_element_type=jnp.float32
        )
        out[mine, :] = total[mine, k * rows : (k + 1) * rows] + part


def finish(k, pieces, right, total):
    wide, rows = pieces[0].shape
    vmem = pl.BlockSpec(memory_space=pltpu.VMEM)
    return pl.pallas_call(
        functools.partial(finish_kernel, k),
        out_shape=jax.ShapeDtypeStruct((2 * wide, rows), jnp.float32),
        in_specs=[vmem] * 4,
        out_specs=vmem,
        cost_estimate=pl.CostEstimate(flops=12 * rows * rows * wide, bytes_accessed=16 * rows * rows, transcendentals=0),
        compiler_params=pltpu.CompilerParams(vmem_limit_bytes=DOTS_LIMIT),
        name="finish",
    )(*pieces, right, total)


def take_kernel(core, block, gmap, *outs):
    rows, width = block.shape
    quarter = width // 4
    pick = (lax.broadcasted_iota(jnp.int32, (rows, rows), 0) == gmap[...]).astype(jnp.bfloat16)
    pick = jnp.concatenate([pick, pick, pick], 0)
    for at in range(4):
        col = jnp.where(core[0] == 0, at, (at + 2) % 4) * quarter
        x = block[:, pl.ds(pl.multiple_of(col, quarter), quarter)].T
        high, rest = split(x)
        rest = x - high.astype(jnp.float32)
        mid, low = split(rest)
        got = jnp.dot(jnp.concatenate([high, mid, low], 1), pick, preferred_element_type=jnp.float32)
        if at < 2:
            outs[at][...] = got
        else:
            outs[2][(at - 2) * quarter : (at - 1) * quarter, :] = got


def take(core, pair_elements, local_rows):
    rows, width = pair_elements.shape
    piece = jax.ShapeDtypeStruct((width // 4, rows), jnp.float32)
    return pl.pallas_call(
        take_kernel,
        out_shape=(piece, piece, jax.ShapeDtypeStruct((width // 2, rows), jnp.float32)),
        in_specs=[
            pl.BlockSpec(memory_space=pltpu.SMEM),
            pl.BlockSpec(memory_space=pltpu.VMEM),
            pl.BlockSpec(memory_space=pltpu.VMEM),
        ],
        out_specs=[pl.BlockSpec(memory_space=pltpu.VMEM)] * 3,
        cost_estimate=pl.CostEstimate(flops=6 * rows * rows * width, bytes_accessed=8 * rows * width, transcendentals=0),
        compiler_params=pltpu.CompilerParams(vmem_limit_bytes=LIMIT),
        name="take",
    )(core.reshape(1), pair_elements, local_rows.reshape(1, rows))


def turn_kernel(core, x, *refs):
    refs[-1][...] = x[...].T


def turn(at, x, rows, out=None):
    half = x.shape[0]
    more = [] if out is None else [out]
    return pl.pallas_call(
        turn_kernel,
        out_shape=jax.ShapeDtypeStruct((rows, 2 * half), jnp.float32),
        grid_spec=pltpu.PrefetchScalarGridSpec(
            num_scalar_prefetch=1,
            grid=(2,),
            in_specs=[pl.BlockSpec((half // 2, rows), lambda i, c: (i, 0))]
            + [pl.BlockSpec(memory_space=pl.ANY)] * len(more),
            out_specs=pl.BlockSpec((rows, half // 2), lambda i, c: (0, 2 * c[0] + i)),
        ),
        input_output_aliases={2: 0} if more else {},
        compiler_params=pltpu.CompilerParams(vmem_limit_bytes=LIMIT),
        name="turn",
    )(at.reshape(1), x, *more)


def solution(mesh):
    ring = chip_ring(mesh)
    n = len(ring)
    size = 2 * n
    ahead = [(a, b) for i in range(n) for a, b in zip(ring[i], ring[(i + 1) % n])]
    back = [(b, a) for a, b in ahead]
    partner = [(i, i ^ 1) for i in range(size)]
    spot_of = {index: i for i, chip in enumerate(ring) for index in chip}
    sources = [
        [[ring[(spot_of[d] - step * way) % n][0] // 2 for step in range(n)] for way in (1, -1)] for d in range(size)
    ]

    def local(pair_elements, gmap, w_screened, coulomb):
        rows, width = pair_elements.shape
        half = width // 2
        wide = half // 2
        me = lax.axis_index("blk")
        core = me % 2
        source = lax.dynamic_index_in_dim(jnp.array(sources, jnp.int32), me, 0, keepdims=False)
        blocks = (2 * source.T[:, None, :] + ((core + jnp.arange(2)) % 2)[None, :, None]).reshape(n * 4)
        here = core * half
        *mine, away = take(core, pair_elements, lax.rem(gmap, rows))
        given = lax.ppermute(away, "blk", partner)
        w_late, _ = lax.optimization_barrier((w_screened, away))
        w_partner = lax.ppermute(w_late, "blk", partner)
        held = [mine, [given[way * wide : (way + 1) * wide] for way in (0, 1)]]
        start = list(held)

        band = (here + jnp.arange(half, dtype=jnp.int32)) % NB
        coef = jnp.where(band < OCC, -0.5, 0.5).astype(jnp.float32)
        start = [x for pair in start for x in pair]
        total = None
        form = None
        terms = None
        bit_at = size // 2

        def exchange(terms, bit_at):
            bit = (me // bit_at) % 2
            terms = terms.reshape(2, -1)
            keep = jnp.where(bit == 0, terms[0], terms[1])
            send = jnp.where(bit == 0, terms[1], terms[0])
            return keep + lax.ppermute(send, "blk", [(b, b ^ bit_at) for b in range(size)])

        for step in range(n):
            for c in (0, 1):
                if step:
                    held[c] = [lax.ppermute(held[c][way], "blk", back if way else ahead) for way in (0, 1)]
                look = c == 1 and step in (0, n // 2 - 1, n // 2)
                use = held[c]
                if step == n - 1 and c == 1:
                    terms, *use = lax.optimization_barrier((terms, *use))
                    other = finish(1, use, right, total)
                    other = lax.ppermute(other, "blk", partner)
                    own = finish(0, use, right, total)
                    break
                total, seen = dots(blocks, 4 * step + 2 * c, use, w_screened, w_partner, total, start if look else None)
                if step == n - 1:
                    right = fetch(blocks, 4 * step + 2, w_screened, w_partner)
                if look:
                    form = -seen if step == 0 else form + seen
            if step == n // 2:
                own_bare = -0.5 * jnp.sum(jnp.concatenate(mine, 0) ** 2 * coulomb[None, :], axis=1)
                away_bare = -0.5 * jnp.sum(away * away * coulomb[None, :], axis=1)
                form = own_bare + coef * jnp.sum(form, axis=1)
                terms = jnp.where(core == 0, jnp.concatenate([form, away_bare]), jnp.concatenate([away_bare, form]))
                while bit_at:
                    terms = exchange(terms, bit_at)
                    bit_at //= 2
        screened = turn(core, own, rows)
        screened = turn(1 - core, other, rows, screened)
        return screened, terms

    in_specs = (
        P(("groups", "blk"), None),
        P(("groups", "blk")),
        P("groups", "blk"),
        P(("groups", "blk")),
    )
    out_specs = (P(("groups", "blk"), None), P(("groups", "blk")))
    return jax.shard_map(local, mesh=mesh, in_specs=in_specs, out_specs=out_specs, check_vma=False)
```

```python
import functools

import jax
import jax.numpy as jnp
from jax import lax
from jax.experimental import pallas as pl
from jax.experimental.pallas import tpu as pltpu
from jax.sharding import PartitionSpec as P


NB = 64
OCC = 4
LIMIT = 20 << 20
DOTS_LIMIT = 46 << 20


def chip_ring(mesh):
    row = mesh.devices.reshape(mesh.shape["groups"], -1)[0]
    places = [tuple(getattr(d, "coords", (0, 0, i // 2))) for i, d in enumerate(row)]
    chips = {}
    for index, place in enumerate(places):
        chips.setdefault(place, []).append(index)
    ordered = []
    spread = [len({p[k] for p in chips}) for k in range(3)]
    long = max(range(3), key=lambda k: spread[k])
    lanes = {}
    for p in chips:
        lanes.setdefault(tuple(v for k, v in enumerate(p) if k != long), []).append(p)
    for number, lane in enumerate(sorted(lanes)):
        line = sorted(lanes[lane], key=lambda p: p[long])
        ordered += line[::-1] if number % 2 else line
    return [chips[p] for p in ordered]


def split(x):
    high = x.astype(jnp.bfloat16)
    return high, (x - high.astype(jnp.float32)).astype(jnp.bfloat16)


def dots_kernel(at, first, watch, blocks, x0, x1, w_own, w_partner, *refs):
    left, landed, sems = refs[-3:]
    refs = refs[:-3]
    out = refs[-watch - 1]
    rows = landed.shape[1]
    wide = x0.shape[0]

    def copies(way):
        here = pl.ds(pl.multiple_of(blocks[at + way] * rows, rows), rows)
        for k, w in enumerate((w_own, w_partner)):
            yield pltpu.make_async_copy(
                w.at[here], landed.at[way, :, k * rows : (k + 1) * rows], sems.at[way, k]
            )

    for way in (0, 1):
        for copy in copies(way):
            copy.start()
    for way, x in enumerate((x0, x1)):
        xh, xl = split(x[...])
        for i, part in enumerate((xh, xl, xh)):
            left[way, :, i * rows : (i + 1) * rows] = part

    def product(way):
        for copy in copies(way):
            copy.wait()
        wh, wl = split(landed[way])
        total = jnp.dot(left[way], jnp.concatenate([wh, wh, wl], 0), preferred_element_type=jnp.float32)
        mine = pl.ds(way * wide if isinstance(way, int) else pl.multiple_of(way * wide, wide), wide)
        if not first:
            total = refs[0][mine, :] + total
        out[mine, :] = total
        return total

    if watch:
        for way in (0, 1):
            seen = product(way) * jnp.concatenate([refs[1 + way][...], refs[3 + way][...]], 1)
            seen = functools.reduce(lambda p, q: p + q, [seen[:, i : i + 128] for i in range(0, 2 * rows, 128)])
            refs[-1][way * wide : (way + 1) * wide, :] = seen
    else:

        @pl.loop(0, 2)
        def _(way):
            product(way)


def dots(blocks, at, pieces, w_own, w_partner, total=None, start=None):
    wide, rows = pieces[0].shape
    vmem = pl.BlockSpec(memory_space=pltpu.VMEM)
    hbm = pl.BlockSpec(memory_space=pltpu.HBM)
    more = [] if total is None else [total]
    watch = [] if start is None else list(start)
    shape = jax.ShapeDtypeStruct((2 * wide, 2 * rows), jnp.float32)
    form = jax.ShapeDtypeStruct((2 * wide, 128), jnp.float32)
    out = pl.pallas_call(
        functools.partial(dots_kernel, at, total is None, int(start is not None)),
        out_shape=(shape, form) if watch else (shape,),
        in_specs=[pl.BlockSpec(memory_space=pltpu.SMEM), vmem, vmem, hbm, hbm] + [vmem] * (len(more) + len(watch)),
        out_specs=(vmem, vmem)[: 2 if watch else 1],
        scratch_shapes=[
            pltpu.VMEM((2, wide, 3 * rows), jnp.bfloat16),
            pltpu.VMEM((2, rows, 2 * rows), jnp.float32),
            pltpu.SemaphoreType.DMA((2, 2)),
        ],
        input_output_aliases={5: 0} if more else {},
        cost_estimate=pl.CostEstimate(
            flops=24 * rows * rows * wide, bytes_accessed=16 * rows * rows, transcendentals=0
        ),
        compiler_params=pltpu.CompilerParams(vmem_limit_bytes=DOTS_LIMIT),
        name="dots",
    )(blocks, *pieces, w_own, w_partner, *more, *watch)
    return out if watch else (out[0], None)


def fetch_kernel(at, blocks, w_own, w_partner, out, landed, sems):
    rows = landed.shape[1]
    copies = []
    for k, w in enumerate((w_partner, w_own)):
        for way in (0, 1):
            here = pl.ds(pl.multiple_of(blocks[at + way] * rows, rows), rows)
            copies.append(pltpu.make_async_copy(w.at[here], landed.at[2 * k + way], sems.at[2 * k + way]))
    for copy in copies:
        copy.start()
    for i, copy in enumerate(copies):
        copy.wait()
        high, low = split(landed[i])
        out[i] = jnp.concatenate([high, low], 0)


def fetch(blocks, at, w_own, w_partner):
    rows = w_own.shape[1]
    hbm = pl.BlockSpec(memory_space=pltpu.HBM)
    return pl.pallas_call(
        functools.partial(fetch_kernel, at),
        out_shape=jax.ShapeDtypeStruct((4, 2 * rows, rows), jnp.bfloat16),
        in_specs=[pl.BlockSpec(memory_space=pltpu.SMEM), hbm, hbm],
        out_specs=pl.BlockSpec(memory_space=pltpu.VMEM),
        scratch_shapes=[pltpu.VMEM((4, rows, rows), jnp.float32), pltpu.SemaphoreType.DMA((4,))],
        cost_estimate=pl.CostEstimate(flops=8 * rows * rows, bytes_accessed=40 * rows * rows, transcendentals=0),
        compiler_params=pltpu.CompilerParams(vmem_limit_bytes=DOTS_LIMIT),
        name="fetch",
    )(blocks, w_own, w_partner)


def last_part(k, way, x, right, total):
    wide, rows = x.shape
    xh, xl = split(x[...])
    at = 2 * (1 - k) + way
    high, low = right[at, :rows], right[at, rows:]
    part = jnp.dot(
        jnp.concatenate([xh, xl, xh], 1), jnp.concatenate([high, high, low], 0), preferred_element_type=jnp.float32
    )
    return total[way * wide : (way + 1) * wide, k * rows : (k + 1) * rows] + part


def give_kernel(x0, x1, right, total, out):
    wide = x0.shape[0]
    for way, x in enumerate((x0, x1)):
        out[way * wide : (way + 1) * wide, :] = last_part(1, way, x, right, total)


def finish_partner(pieces, right, total):
    wide, rows = pieces[0].shape
    vmem = pl.BlockSpec(memory_space=pltpu.VMEM)
    return pl.pallas_call(
        give_kernel,
        out_shape=jax.ShapeDtypeStruct((2 * wide, rows), jnp.float32),
        in_specs=[vmem] * 4,
        out_specs=vmem,
        cost_estimate=pl.CostEstimate(flops=12 * rows * rows * wide, bytes_accessed=16 * rows * rows, transcendentals=0),
        compiler_params=pltpu.CompilerParams(vmem_limit_bytes=DOTS_LIMIT),
        name="finish",
    )(*pieces, right, total)


def send_out(value, way, base, turned, sems, out):
    wide = value.shape[0]
    turned[way] = value.T
    columns = pl.ds(pl.multiple_of(base + way * wide, wide), wide)
    copy = pltpu.make_async_copy(turned.at[way], out.at[:, columns], sems.at[way])
    copy.start()
    return copy


def own_kernel(core, x0, x1, right, total, out, turned, sems):
    wide = x0.shape[0]
    copies = [
        send_out(last_part(0, way, x, right, total), way, core[0] * 2 * wide, turned, sems, out)
        for way, x in enumerate((x0, x1))
    ]
    for copy in copies:
        copy.wait()


def finish_own(core, pieces, right, total):
    wide, rows = pieces[0].shape
    vmem = pl.BlockSpec(memory_space=pltpu.VMEM)
    return pl.pallas_call(
        own_kernel,
        out_shape=jax.ShapeDtypeStruct((rows, 4 * wide), jnp.float32),
        in_specs=[pl.BlockSpec(memory_space=pltpu.SMEM)] + [vmem] * 4,
        out_specs=pl.BlockSpec(memory_space=pl.ANY),
        scratch_shapes=[pltpu.VMEM((2, rows, wide), jnp.float32), pltpu.SemaphoreType.DMA((2,))],
        cost_estimate=pl.CostEstimate(flops=12 * rows * rows * wide, bytes_accessed=16 * rows * rows, transcendentals=0),
        compiler_params=pltpu.CompilerParams(vmem_limit_bytes=DOTS_LIMIT),
        name="finish_own",
    )(core.reshape(1), *pieces, right, total)


def other_kernel(core, x, _, out, turned, sems):
    wide = turned.shape[2]
    count = turned.shape[0]
    copies = [
        send_out(x[i * wide : (i + 1) * wide, :], i, (1 - core[0]) * count * wide, turned, sems, out)
        for i in range(count)
    ]
    for copy in copies:
        copy.wait()


def place_other(core, other, out):
    half, rows = other.shape
    return pl.pallas_call(
        other_kernel,
        out_shape=jax.ShapeDtypeStruct((rows, 2 * half), jnp.float32),
        in_specs=[
            pl.BlockSpec(memory_space=pltpu.SMEM),
            pl.BlockSpec(memory_space=pltpu.VMEM),
            pl.BlockSpec(memory_space=pl.ANY),
        ],
        out_specs=pl.BlockSpec(memory_space=pl.ANY),
        scratch_shapes=[pltpu.VMEM((4, rows, half // 4), jnp.float32), pltpu.SemaphoreType.DMA((4,))],
        input_output_aliases={2: 0},
        compiler_params=pltpu.CompilerParams(vmem_limit_bytes=DOTS_LIMIT),
        name="place",
    )(core.reshape(1), other, out)


def take_kernel(core, block, gmap, *outs):
    rows, width = block.shape
    quarter = width // 4
    pick = (lax.broadcasted_iota(jnp.int32, (rows, rows), 0) == lax.rem(gmap[...], rows)[None, :]).astype(jnp.bfloat16)
    pick = jnp.concatenate([pick, pick, pick], 0)
    for at in range(4):
        col = jnp.where(core[0] == 0, at, (at + 2) % 4) * quarter
        x = block[:, pl.ds(pl.multiple_of(col, quarter), quarter)].T
        high, rest = split(x)
        rest = x - high.astype(jnp.float32)
        mid, low = split(rest)
        got = jnp.dot(jnp.concatenate([high, mid, low], 1), pick, preferred_element_type=jnp.float32)
        if at < 2:
            outs[at][...] = got
        else:
            outs[2][(at - 2) * quarter : (at - 1) * quarter, :] = got


def take(core, pair_elements, gmap):
    rows, width = pair_elements.shape
    piece = jax.ShapeDtypeStruct((width // 4, rows), jnp.float32)
    return pl.pallas_call(
        take_kernel,
        out_shape=(piece, piece, jax.ShapeDtypeStruct((width // 2, rows), jnp.float32)),
        in_specs=[
            pl.BlockSpec(memory_space=pltpu.SMEM),
            pl.BlockSpec(memory_space=pltpu.VMEM),
            pl.BlockSpec(memory_space=pltpu.VMEM),
        ],
        out_specs=[pl.BlockSpec(memory_space=pltpu.VMEM)] * 3,
        cost_estimate=pl.CostEstimate(flops=6 * rows * rows * width, bytes_accessed=8 * rows * width, transcendentals=0),
        compiler_params=pltpu.CompilerParams(vmem_limit_bytes=LIMIT),
        name="take",
    )(core.reshape(1), pair_elements, gmap)


def solution(mesh):
    ring = chip_ring(mesh)
    n = len(ring)
    size = 2 * n
    ahead = [(a, b) for i in range(n) for a, b in zip(ring[i], ring[(i + 1) % n])]
    back = [(b, a) for a, b in ahead]
    partner = [(i, i ^ 1) for i in range(size)]
    spot_of = {index: i for i, chip in enumerate(ring) for index in chip}
    sources = [
        [[ring[(spot_of[d] - step * way) % n][0] // 2 for step in range(n)] for way in (1, -1)] for d in range(size)
    ]

    def local(pair_elements, gmap, w_screened, coulomb):
        _, width = pair_elements.shape
        half = width // 2
        wide = half // 2
        me = lax.axis_index("blk")
        core = me % 2
        source = lax.dynamic_index_in_dim(jnp.array(sources, jnp.int32), me, 0, keepdims=False)
        blocks = (2 * source.T[:, None, :] + ((core + jnp.arange(2)) % 2)[None, :, None]).reshape(n * 4)
        here = core * half
        *mine, away = take(core, pair_elements, gmap)
        given = lax.ppermute(away, "blk", partner)
        w_late, _ = lax.optimization_barrier((w_screened, away))
        w_partner = lax.ppermute(w_late, "blk", partner)
        held = [mine, [given[way * wide : (way + 1) * wide] for way in (0, 1)]]
        start = list(held)

        band = (here + jnp.arange(half, dtype=jnp.int32)) % NB
        coef = jnp.where(band < OCC, -0.5, 0.5).astype(jnp.float32)
        start = [x for pair in start for x in pair]
        total = None
        form = None
        terms = None
        bit_at = size // 2

        def exchange(terms, bit_at):
            bit = (me // bit_at) % 2
            terms = terms.reshape(2, -1)
            keep = jnp.where(bit == 0, terms[0], terms[1])
            send = jnp.where(bit == 0, terms[1], terms[0])
            return keep + lax.ppermute(send, "blk", [(b, b ^ bit_at) for b in range(size)])

        for step in range(n):
            for c in (0, 1):
                if step:
                    held[c] = [lax.ppermute(held[c][way], "blk", back if way else ahead) for way in (0, 1)]
                look = c == 1 and step in (0, n // 2 - 1, n // 2)
                use = held[c]
                if step == n - 1 and c == 1:
                    terms, *use = lax.optimization_barrier((terms, *use))
                    other = finish_partner(use, right, total)
                    other = lax.ppermute(other, "blk", partner)
                    screened = finish_own(core, use, right, total)
                    break
                total, seen = dots(blocks, 4 * step + 2 * c, use, w_screened, w_partner, total, start if look else None)
                if step == n - 1:
                    right = fetch(blocks, 4 * step + 2, w_screened, w_partner)
                if look:
                    form = -seen if step == 0 else form + seen
            if step == n // 2:
                own_bare = -0.5 * jnp.sum(jnp.concatenate(mine, 0) ** 2 * coulomb[None, :], axis=1)
                away_bare = -0.5 * jnp.sum(away * away * coulomb[None, :], axis=1)
                form = own_bare + coef * jnp.sum(form, axis=1)
                terms = jnp.where(core == 0, jnp.concatenate([form, away_bare]), jnp.concatenate([away_bare, form]))
                while bit_at:
                    terms = exchange(terms, bit_at)
                    bit_at //= 2
        screened = place_other(core, other, screened)
        return screened, terms

    in_specs = (
        P(("groups", "blk"), None),
        P(("groups", "blk")),
        P("groups", "blk"),
        P(("groups", "blk")),
    )
    out_specs = (P(("groups", "blk"), None), P(("groups", "blk")))
    return jax.shard_map(local, mesh=mesh, in_specs=in_specs, out_specs=out_specs, check_vma=False)
```

```python
import functools

import jax
import jax.numpy as jnp
from jax import lax
from jax.experimental import pallas as pl
from jax.experimental.pallas import tpu as pltpu
from jax.sharding import PartitionSpec as P


NB = 64
OCC = 4
LIMIT = 20 << 20
DOTS_LIMIT = 46 << 20


def chip_ring(mesh):
    row = mesh.devices.reshape(mesh.shape["groups"], -1)[0]
    places = [tuple(getattr(d, "coords", (0, 0, i // 2))) for i, d in enumerate(row)]
    chips = {}
    for index, place in enumerate(places):
        chips.setdefault(place, []).append(index)
    ordered = []
    spread = [len({p[k] for p in chips}) for k in range(3)]
    long = max(range(3), key=lambda k: spread[k])
    lanes = {}
    for p in chips:
        lanes.setdefault(tuple(v for k, v in enumerate(p) if k != long), []).append(p)
    for number, lane in enumerate(sorted(lanes)):
        line = sorted(lanes[lane], key=lambda p: p[long])
        ordered += line[::-1] if number % 2 else line
    return [chips[p] for p in ordered]


def split(x):
    high = x.astype(jnp.bfloat16)
    return high, (x - high.astype(jnp.float32)).astype(jnp.bfloat16)


def dots_kernel(at, first, watch, blocks, x0, x1, w_own, w_partner, *refs):
    left, landed, sems = refs[-3:]
    refs = refs[:-3]
    out = refs[-watch - 1]
    rows = landed.shape[1]
    wide = x0.shape[0]

    def copies(way):
        here = pl.ds(pl.multiple_of(blocks[at + way] * rows, rows), rows)
        for k, w in enumerate((w_own, w_partner)):
            yield pltpu.make_async_copy(
                w.at[here], landed.at[way, :, k * rows : (k + 1) * rows], sems.at[way, k]
            )

    for way in (0, 1):
        for copy in copies(way):
            copy.start()
    for way, x in enumerate((x0, x1)):
        xh, xl = split(x[...])
        for i, part in enumerate((xh, xl, xh)):
            left[way, :, i * rows : (i + 1) * rows] = part

    def product(way):
        for copy in copies(way):
            copy.wait()
        wh, wl = split(landed[way])
        total = jnp.dot(left[way], jnp.concatenate([wh, wh, wl], 0), preferred_element_type=jnp.float32)
        mine = pl.ds(way * wide if isinstance(way, int) else pl.multiple_of(way * wide, wide), wide)
        if not first:
            total = refs[0][mine, :] + total
        out[mine, :] = total
        return total

    if watch:
        for way in (0, 1):
            seen = product(way) * jnp.concatenate([refs[1 + way][...], refs[3 + way][...]], 1)
            seen = functools.reduce(lambda p, q: p + q, [seen[:, i : i + 128] for i in range(0, 2 * rows, 128)])
            refs[-1][way * wide : (way + 1) * wide, :] = seen
    else:

        @pl.loop(0, 2)
        def _(way):
            product(way)


def dots(blocks, at, pieces, w_own, w_partner, total=None, start=None):
    wide, rows = pieces[0].shape
    vmem = pl.BlockSpec(memory_space=pltpu.VMEM)
    hbm = pl.BlockSpec(memory_space=pltpu.HBM)
    more = [] if total is None else [total]
    watch = [] if start is None else list(start)
    shape = jax.ShapeDtypeStruct((2 * wide, 2 * rows), jnp.float32)
    form = jax.ShapeDtypeStruct((2 * wide, 128), jnp.float32)
    out = pl.pallas_call(
        functools.partial(dots_kernel, at, total is None, int(start is not None)),
        out_shape=(shape, form) if watch else (shape,),
        in_specs=[pl.BlockSpec(memory_space=pltpu.SMEM), vmem, vmem, hbm, hbm] + [vmem] * (len(more) + len(watch)),
        out_specs=(vmem, vmem)[: 2 if watch else 1],
        scratch_shapes=[
            pltpu.VMEM((2, wide, 3 * rows), jnp.bfloat16),
            pltpu.VMEM((2, rows, 2 * rows), jnp.float32),
            pltpu.SemaphoreType.DMA((2, 2)),
        ],
        input_output_aliases={5: 0} if more else {},
        cost_estimate=pl.CostEstimate(
            flops=24 * rows * rows * wide, bytes_accessed=16 * rows * rows, transcendentals=0
        ),
        compiler_params=pltpu.CompilerParams(vmem_limit_bytes=DOTS_LIMIT),
        name="dots",
    )(blocks, *pieces, w_own, w_partner, *more, *watch)
    return out if watch else (out[0], None)


def fetch_kernel(at, blocks, w_own, w_partner, out, landed, sems):
    rows = landed.shape[1]
    copies = []
    for k, w in enumerate((w_partner, w_own)):
        for way in (0, 1):
            here = pl.ds(pl.multiple_of(blocks[at + way] * rows, rows), rows)
            copies.append(pltpu.make_async_copy(w.at[here], landed.at[2 * k + way], sems.at[2 * k + way]))
    for copy in copies:
        copy.start()
    for i, copy in enumerate(copies):
        copy.wait()
        high, low = split(landed[i])
        out[i] = jnp.concatenate([high, low], 0)


def fetch(blocks, at, w_own, w_partner):
    rows = w_own.shape[1]
    hbm = pl.BlockSpec(memory_space=pltpu.HBM)
    return pl.pallas_call(
        functools.partial(fetch_kernel, at),
        out_shape=jax.ShapeDtypeStruct((4, 2 * rows, rows), jnp.bfloat16),
        in_specs=[pl.BlockSpec(memory_space=pltpu.SMEM), hbm, hbm],
        out_specs=pl.BlockSpec(memory_space=pltpu.VMEM),
        scratch_shapes=[pltpu.VMEM((4, rows, rows), jnp.float32), pltpu.SemaphoreType.DMA((4,))],
        cost_estimate=pl.CostEstimate(flops=8 * rows * rows, bytes_accessed=40 * rows * rows, transcendentals=0),
        compiler_params=pltpu.CompilerParams(vmem_limit_bytes=DOTS_LIMIT),
        name="fetch",
    )(blocks, w_own, w_partner)


def last_part(k, way, x, right, total):
    wide, rows = x.shape
    xh, xl = split(x[...])
    at = 2 * (1 - k) + way
    high, low = right[at, :rows], right[at, rows:]
    part = jnp.dot(
        jnp.concatenate([xh, xl, xh], 1), jnp.concatenate([high, high, low], 0), preferred_element_type=jnp.float32
    )
    return total[way * wide : (way + 1) * wide, k * rows : (k + 1) * rows] + part


def give_kernel(x0, x1, right, total, out):
    wide = x0.shape[0]
    for way, x in enumerate((x0, x1)):
        out[way * wide : (way + 1) * wide, :] = last_part(1, way, x, right, total)


def finish_partner(pieces, right, total):
    wide, rows = pieces[0].shape
    vmem = pl.BlockSpec(memory_space=pltpu.VMEM)
    return pl.pallas_call(
        give_kernel,
        out_shape=jax.ShapeDtypeStruct((2 * wide, rows), jnp.float32),
        in_specs=[vmem] * 4,
        out_specs=vmem,
        cost_estimate=pl.CostEstimate(flops=12 * rows * rows * wide, bytes_accessed=16 * rows * rows, transcendentals=0),
        compiler_params=pltpu.CompilerParams(vmem_limit_bytes=DOTS_LIMIT),
        name="finish",
    )(*pieces, right, total)


def send_out(value, way, base, turned, sems, out):
    wide = value.shape[0]
    turned[way] = value.T
    columns = pl.ds(pl.multiple_of(base + way * wide, wide), wide)
    copy = pltpu.make_async_copy(turned.at[way], out.at[:, columns], sems.at[way])
    copy.start()
    return copy


def own_kernel(core, x0, x1, right, total, out, turned, sems):
    wide = x0.shape[0]
    copies = [
        send_out(last_part(0, way, x, right, total), way, core[0] * 2 * wide, turned, sems, out)
        for way, x in enumerate((x0, x1))
    ]
    for copy in copies:
        copy.wait()


def finish_own(core, pieces, right, total):
    wide, rows = pieces[0].shape
    vmem = pl.BlockSpec(memory_space=pltpu.VMEM)
    return pl.pallas_call(
        own_kernel,
        out_shape=jax.ShapeDtypeStruct((rows, 4 * wide), jnp.float32),
        in_specs=[pl.BlockSpec(memory_space=pltpu.SMEM)] + [vmem] * 4,
        out_specs=pl.BlockSpec(memory_space=pl.ANY),
        scratch_shapes=[pltpu.VMEM((2, rows, wide), jnp.float32), pltpu.SemaphoreType.DMA((2,))],
        cost_estimate=pl.CostEstimate(flops=12 * rows * rows * wide, bytes_accessed=16 * rows * rows, transcendentals=0),
        compiler_params=pltpu.CompilerParams(vmem_limit_bytes=DOTS_LIMIT),
        name="finish_own",
    )(core.reshape(1), *pieces, right, total)


def other_kernel(core, x, _, out, turned, sems):
    wide = turned.shape[2]
    count = turned.shape[0]
    copies = [
        send_out(x[i * wide : (i + 1) * wide, :], i, (1 - core[0]) * count * wide, turned, sems, out)
        for i in range(count)
    ]
    for copy in copies:
        copy.wait()


def place_other(core, other, out):
    half, rows = other.shape
    return pl.pallas_call(
        other_kernel,
        out_shape=jax.ShapeDtypeStruct((rows, 2 * half), jnp.float32),
        in_specs=[
            pl.BlockSpec(memory_space=pltpu.SMEM),
            pl.BlockSpec(memory_space=pltpu.VMEM),
            pl.BlockSpec(memory_space=pl.ANY),
        ],
        out_specs=pl.BlockSpec(memory_space=pl.ANY),
        scratch_shapes=[pltpu.VMEM((4, rows, half // 4), jnp.float32), pltpu.SemaphoreType.DMA((4,))],
        input_output_aliases={2: 0},
        compiler_params=pltpu.CompilerParams(vmem_limit_bytes=DOTS_LIMIT),
        name="place",
    )(core.reshape(1), other, out)


def take_kernel(side, block, gmap, *refs):
    outs, landed, order, sems = refs[:-3], refs[-3], refs[-2], refs[-1]
    rows, width = block.shape
    quarter = width // 4
    copies = []
    for at in (0, 1):
        columns = pl.ds(pl.multiple_of((2 * side[0] + at) * quarter, quarter), quarter)
        copies.append(pltpu.make_async_copy(block.at[:, columns], landed.at[at], sems.at[at]))
    ordered = pltpu.make_async_copy(gmap, order, sems.at[2])
    for copy in (copies[0], ordered, copies[1]):
        copy.start()
    ordered.wait()
    pick = (lax.broadcasted_iota(jnp.int32, (rows, rows), 0) == lax.rem(order[...], rows)[None, :]).astype(jnp.bfloat16)
    pick = jnp.concatenate([pick, pick, pick], 0)
    for at in (0, 1):
        copies[at].wait()
        x = landed[at].T
        high, rest = split(x)
        rest = x - high.astype(jnp.float32)
        mid, low = split(rest)
        got = jnp.dot(jnp.concatenate([high, mid, low], 1), pick, preferred_element_type=jnp.float32)
        if len(outs) == 2:
            outs[at][...] = got
        else:
            outs[0][at * quarter : (at + 1) * quarter, :] = got


def take(side, pair_elements, gmap, pieces):
    rows, width = pair_elements.shape
    piece = jax.ShapeDtypeStruct((width // 2 // pieces, rows), jnp.float32)
    hbm = pl.BlockSpec(memory_space=pltpu.HBM)
    return pl.pallas_call(
        take_kernel,
        out_shape=(piece,) * pieces,
        in_specs=[pl.BlockSpec(memory_space=pltpu.SMEM), hbm, hbm],
        out_specs=(pl.BlockSpec(memory_space=pltpu.VMEM),) * pieces,
        scratch_shapes=[
            pltpu.VMEM((2, rows, width // 4), jnp.float32),
            pltpu.VMEM((rows,), jnp.int32),
            pltpu.SemaphoreType.DMA((3,)),
        ],
        cost_estimate=pl.CostEstimate(flops=3 * rows * rows * width, bytes_accessed=4 * rows * width, transcendentals=0),
        compiler_params=pltpu.CompilerParams(vmem_limit_bytes=LIMIT),
        name="take",
    )(side.reshape(1), *(pltpu.with_memory_space_constraint(x, pltpu.HBM) for x in (pair_elements, gmap)))


def solution(mesh):
    ring = chip_ring(mesh)
    n = len(ring)
    size = 2 * n
    ahead = [(a, b) for i in range(n) for a, b in zip(ring[i], ring[(i + 1) % n])]
    back = [(b, a) for a, b in ahead]
    partner = [(i, i ^ 1) for i in range(size)]
    spot_of = {index: i for i, chip in enumerate(ring) for index in chip}
    sources = [
        [[ring[(spot_of[d] - step * way) % n][0] // 2 for step in range(n)] for way in (1, -1)] for d in range(size)
    ]

    bits = [1 << i for i in range(size.bit_length() - 1)]
    phases = [(bit,) for bit in bits[:-2]] + [(bits[-1], bits[-2])]

    def local(pair_elements, gmap, w_screened, coulomb):
        _, width = pair_elements.shape
        half = width // 2
        wide = half // 2
        me = lax.axis_index("blk")
        core = me % 2
        source = lax.dynamic_index_in_dim(jnp.array(sources, jnp.int32), me, 0, keepdims=False)
        blocks = (2 * source.T[:, None, :] + ((core + jnp.arange(2)) % 2)[None, :, None]).reshape(n * 4)
        here = core * half
        mine = list(take(core, pair_elements, gmap, 2))
        (away,) = take(1 - core, pair_elements, gmap, 1)
        given = lax.ppermute(away, "blk", partner)
        w_late, _ = lax.optimization_barrier((w_screened, away))
        w_partner = lax.ppermute(w_late, "blk", partner)
        held = [mine, [given[way * wide : (way + 1) * wide] for way in (0, 1)]]
        start = list(held)

        band = (here + jnp.arange(half, dtype=jnp.int32)) % NB
        coef = jnp.where(band < OCC, -0.5, 0.5).astype(jnp.float32)
        start = [x for pair in start for x in pair]
        total = None
        form = None
        terms = None

        def exchange(terms, bits, left):
            at = [left.index(bit) for bit in bits]
            terms = terms.reshape((2,) * len(left) + (-1,))
            terms = jnp.moveaxis(terms, at, range(len(at))).reshape(1 << len(at), -1)
            mine = sum(((me // bit) % 2) << (len(bits) - 1 - i) for i, bit in enumerate(bits))
            kept = lax.dynamic_index_in_dim(terms, mine, 0, keepdims=False)
            for x in range(1, 1 << len(bits)):
                mask = sum(bit for i, bit in enumerate(bits) if (x >> (len(bits) - 1 - i)) & 1)
                sent = lax.dynamic_index_in_dim(terms, mine ^ x, 0, keepdims=False)
                kept = kept + lax.ppermute(sent, "blk", [(b, b ^ mask) for b in range(size)])
            return kept

        for step in range(n):
            for c in (0, 1):
                if step:
                    held[c] = [lax.ppermute(held[c][way], "blk", back if way else ahead) for way in (0, 1)]
                look = c == 1 and step in (0, n // 2 - 1, n // 2)
                use = held[c]
                if step == n - 1 and c == 1:
                    terms, *use = lax.optimization_barrier((terms, *use))
                    other = finish_partner(use, right, total)
                    other = lax.ppermute(other, "blk", partner)
                    screened = finish_own(core, use, right, total)
                    break
                total, seen = dots(blocks, 4 * step + 2 * c, use, w_screened, w_partner, total, start if look else None)
                if step == n - 1:
                    right = fetch(blocks, 4 * step + 2, w_screened, w_partner)
                if look:
                    form = -seen if step == 0 else form + seen
            if step == n // 2:
                own_bare = -0.5 * jnp.sum(jnp.concatenate(mine, 0) ** 2 * coulomb[None, :], axis=1)
                away_bare = -0.5 * jnp.sum(away * away * coulomb[None, :], axis=1)
                form = own_bare + coef * jnp.sum(form, axis=1)
                terms = jnp.where(core == 0, jnp.concatenate([form, away_bare]), jnp.concatenate([away_bare, form]))
                left = [bit for phase in reversed(phases) for bit in phase]
                for phase in phases:
                    terms = exchange(terms, phase, left)
                    left = [bit for bit in left if bit not in phase]
        screened = place_other(core, other, screened)
        return screened, terms

    in_specs = (
        P(("groups", "blk"), None),
        P(("groups", "blk")),
        P("groups", "blk"),
        P(("groups", "blk")),
    )
    out_specs = (P(("groups", "blk"), None), P(("groups", "blk")))
    return jax.shard_map(local, mesh=mesh, in_specs=in_specs, out_specs=out_specs, check_vma=False)
```

```python
import functools

import jax
import jax.numpy as jnp
from jax import lax
from jax.experimental import pallas as pl
from jax.experimental.pallas import tpu as pltpu
from jax.sharding import PartitionSpec as P


NB = 64
OCC = 4
PARTS = 2
LIMIT = 20 << 20
DOTS_LIMIT = 46 << 20


def chip_ring(mesh):
    row = mesh.devices.reshape(mesh.shape["groups"], -1)[0]
    places = [tuple(getattr(d, "coords", (0, 0, i // 2))) for i, d in enumerate(row)]
    chips = {}
    for index, place in enumerate(places):
        chips.setdefault(place, []).append(index)
    ordered = []
    spread = [len({p[k] for p in chips}) for k in range(3)]
    long = max(range(3), key=lambda k: spread[k])
    lanes = {}
    for p in chips:
        lanes.setdefault(tuple(v for k, v in enumerate(p) if k != long), []).append(p)
    for number, lane in enumerate(sorted(lanes)):
        line = sorted(lanes[lane], key=lambda p: p[long])
        ordered += line[::-1] if number % 2 else line
    return [chips[p] for p in ordered]


def split(x):
    high = x.astype(jnp.bfloat16)
    return high, (x - high.astype(jnp.float32)).astype(jnp.bfloat16)


def dots_kernel(at, first, watch, blocks, x0, x1, w_own, w_partner, *refs):
    left, landed, sems = refs[-3:]
    refs = refs[:-3]
    out = refs[-watch - 1]
    rows = landed.shape[1]
    wide = x0.shape[0]

    def copies(way):
        here = pl.ds(pl.multiple_of(blocks[at + way] * rows, rows), rows)
        for k, w in enumerate((w_own, w_partner)):
            yield pltpu.make_async_copy(
                w.at[here], landed.at[way, :, k * rows : (k + 1) * rows], sems.at[way, k]
            )

    for way in (0, 1):
        for copy in copies(way):
            copy.start()
    for way, x in enumerate((x0, x1)):
        xh, xl = split(x[...])
        for i, part in enumerate((xh, xl, xh)):
            left[way, :, i * rows : (i + 1) * rows] = part

    def product(way):
        for copy in copies(way):
            copy.wait()
        wh, wl = split(landed[way])
        total = jnp.dot(left[way], jnp.concatenate([wh, wh, wl], 0), preferred_element_type=jnp.float32)
        mine = pl.ds(way * wide if isinstance(way, int) else pl.multiple_of(way * wide, wide), wide)
        if not first:
            total = refs[0][mine, :] + total
        out[mine, :] = total
        return total

    if watch:
        for way in (0, 1):
            seen = product(way) * jnp.concatenate([refs[1 + way][...], refs[3 + way][...]], 1)
            seen = functools.reduce(lambda p, q: p + q, [seen[:, i : i + 128] for i in range(0, 2 * rows, 128)])
            refs[-1][way * wide : (way + 1) * wide, :] = seen
    else:

        @pl.loop(0, 2)
        def _(way):
            product(way)


def dots(blocks, at, pieces, w_own, w_partner, total=None, start=None):
    wide, rows = pieces[0].shape
    vmem = pl.BlockSpec(memory_space=pltpu.VMEM)
    hbm = pl.BlockSpec(memory_space=pltpu.HBM)
    more = [] if total is None else [total]
    watch = [] if start is None else list(start)
    shape = jax.ShapeDtypeStruct((2 * wide, 2 * rows), jnp.float32)
    form = jax.ShapeDtypeStruct((2 * wide, 128), jnp.float32)
    out = pl.pallas_call(
        functools.partial(dots_kernel, at, total is None, int(start is not None)),
        out_shape=(shape, form) if watch else (shape,),
        in_specs=[pl.BlockSpec(memory_space=pltpu.SMEM), vmem, vmem, hbm, hbm] + [vmem] * (len(more) + len(watch)),
        out_specs=(vmem, vmem)[: 2 if watch else 1],
        scratch_shapes=[
            pltpu.VMEM((2, wide, 3 * rows), jnp.bfloat16),
            pltpu.VMEM((2, rows, 2 * rows), jnp.float32),
            pltpu.SemaphoreType.DMA((2, 2)),
        ],
        input_output_aliases={5: 0} if more else {},
        cost_estimate=pl.CostEstimate(
            flops=24 * rows * rows * wide, bytes_accessed=16 * rows * rows, transcendentals=0
        ),
        compiler_params=pltpu.CompilerParams(vmem_limit_bytes=DOTS_LIMIT),
        name="dots",
    )(blocks, *pieces, w_own, w_partner, *more, *watch)
    return out if watch else (out[0], None)


def fetch_kernel(at, blocks, w_own, w_partner, out, landed, sems):
    rows = landed.shape[1]
    copies = []
    for k, w in enumerate((w_partner, w_own)):
        for way in (0, 1):
            here = pl.ds(pl.multiple_of(blocks[at + way] * rows, rows), rows)
            copies.append(pltpu.make_async_copy(w.at[here], landed.at[2 * k + way], sems.at[2 * k + way]))
    for copy in copies:
        copy.start()
    for i, copy in enumerate(copies):
        copy.wait()
        high, low = split(landed[i])
        out[i] = jnp.concatenate([high, low], 0)


def fetch(blocks, at, w_own, w_partner):
    rows = w_own.shape[1]
    hbm = pl.BlockSpec(memory_space=pltpu.HBM)
    return pl.pallas_call(
        functools.partial(fetch_kernel, at),
        out_shape=jax.ShapeDtypeStruct((4, 2 * rows, rows), jnp.bfloat16),
        in_specs=[pl.BlockSpec(memory_space=pltpu.SMEM), hbm, hbm],
        out_specs=pl.BlockSpec(memory_space=pltpu.VMEM),
        scratch_shapes=[pltpu.VMEM((4, rows, rows), jnp.float32), pltpu.SemaphoreType.DMA((4,))],
        cost_estimate=pl.CostEstimate(flops=8 * rows * rows, bytes_accessed=40 * rows * rows, transcendentals=0),
        compiler_params=pltpu.CompilerParams(vmem_limit_bytes=DOTS_LIMIT),
        name="fetch",
    )(blocks, w_own, w_partner)


def last_part(k, at, way, x, right, total):
    wide, rows = x.shape
    xh, xl = split(x[...])
    block = 2 * (1 - k) + way
    high, low = right[block, :rows], right[block, rows:]
    part = jnp.dot(
        jnp.concatenate([xh, xl, xh], 1), jnp.concatenate([high, high, low], 0), preferred_element_type=jnp.float32
    )
    top = way * total.shape[0] // 2 + at * wide
    return total[top : top + wide, k * rows : (k + 1) * rows] + part


def partner_kernel(at, x0, x1, right, total, out):
    wide = x0.shape[0]
    for way, x in enumerate((x0, x1)):
        out[way * wide : (way + 1) * wide, :] = last_part(1, at, way, x, right, total)


def finish_partner(at, pieces, right, total):
    wide, rows = pieces[0].shape
    vmem = pl.BlockSpec(memory_space=pltpu.VMEM)
    return pl.pallas_call(
        functools.partial(partner_kernel, at),
        out_shape=jax.ShapeDtypeStruct((2 * wide, rows), jnp.float32),
        in_specs=[vmem] * 4,
        out_specs=vmem,
        cost_estimate=pl.CostEstimate(flops=12 * rows * rows * wide, bytes_accessed=16 * rows * rows, transcendentals=0),
        compiler_params=pltpu.CompilerParams(vmem_limit_bytes=DOTS_LIMIT),
        name="finish",
    )(*pieces, right, total)


def send_out(value, half, way, at, turned, sems, out):
    wide = value.shape[0]
    turned[way, at] = value.T
    quarter = out.shape[1] // 4
    columns = pl.ds(pl.multiple_of((2 * half + way) * quarter + at * wide, wide), wide)
    copy = pltpu.make_async_copy(turned.at[way, at], out.at[:, columns], sems.at[way, at])
    copy.start()
    return copy


def own_kernel(core, *refs):
    late, right, total, out, turned, sems = refs[:-5], *refs[-5:]
    copies = [
        send_out(last_part(0, i // 2, i % 2, x, right, total), core[0], i % 2, i // 2, turned, sems, out)
        for i, x in enumerate(late)
    ]
    for copy in copies:
        copy.wait()


def finish_own(core, late, right, total):
    wide, rows = late[0].shape
    vmem = pl.BlockSpec(memory_space=pltpu.VMEM)
    return pl.pallas_call(
        own_kernel,
        out_shape=jax.ShapeDtypeStruct((rows, 2 * total.shape[0]), jnp.float32),
        in_specs=[pl.BlockSpec(memory_space=pltpu.SMEM)] + [vmem] * (len(late) + 2),
        out_specs=pl.BlockSpec(memory_space=pl.ANY),
        scratch_shapes=[pltpu.VMEM((2, PARTS, rows, wide), jnp.float32), pltpu.SemaphoreType.DMA((2, PARTS))],
        cost_estimate=pl.CostEstimate(flops=24 * rows * rows * wide, bytes_accessed=16 * rows * rows, transcendentals=0),
        compiler_params=pltpu.CompilerParams(vmem_limit_bytes=DOTS_LIMIT),
        name="finish_own",
    )(core.reshape(1), *late, right, total)


def place_kernel(core, *refs):
    others, out, turned, sems = refs[:PARTS], *refs[-3:]
    wide = turned.shape[3]
    copies = [
        send_out(x[way * wide : (way + 1) * wide, :], 1 - core[0], way, at, turned, sems, out)
        for at, x in enumerate(others)
        for way in (0, 1)
    ]
    for copy in copies:
        copy.wait()


def place(core, others, out):
    both, rows = others[0].shape
    return pl.pallas_call(
        place_kernel,
        out_shape=jax.ShapeDtypeStruct(out.shape, jnp.float32),
        in_specs=[pl.BlockSpec(memory_space=pltpu.SMEM)]
        + [pl.BlockSpec(memory_space=pltpu.VMEM)] * PARTS
        + [pl.BlockSpec(memory_space=pl.ANY)],
        out_specs=pl.BlockSpec(memory_space=pl.ANY),
        scratch_shapes=[pltpu.VMEM((2, PARTS, rows, both // 2), jnp.float32), pltpu.SemaphoreType.DMA((2, PARTS))],
        input_output_aliases={1 + PARTS: 0},
        compiler_params=pltpu.CompilerParams(vmem_limit_bytes=DOTS_LIMIT),
        name="place",
    )(core.reshape(1), *others, out)


def take_kernel(side, block, gmap, *refs):
    outs, landed, order, sems = refs[:-3], refs[-3], refs[-2], refs[-1]
    rows, width = block.shape
    quarter = width // 4
    copies = []
    for at in (0, 1):
        columns = pl.ds(pl.multiple_of((2 * side[0] + at) * quarter, quarter), quarter)
        copies.append(pltpu.make_async_copy(block.at[:, columns], landed.at[at], sems.at[at]))
    ordered = pltpu.make_async_copy(gmap, order, sems.at[2])
    for copy in (copies[0], ordered, copies[1]):
        copy.start()
    ordered.wait()
    pick = (lax.broadcasted_iota(jnp.int32, (rows, rows), 0) == lax.rem(order[...], rows)[None, :]).astype(jnp.bfloat16)
    pick = jnp.concatenate([pick, pick, pick], 0)
    for at in (0, 1):
        copies[at].wait()
        x = landed[at].T
        high, rest = split(x)
        rest = x - high.astype(jnp.float32)
        mid, low = split(rest)
        got = jnp.dot(jnp.concatenate([high, mid, low], 1), pick, preferred_element_type=jnp.float32)
        if len(outs) == 2:
            outs[at][...] = got
        else:
            outs[0][at * quarter : (at + 1) * quarter, :] = got


def take(side, pair_elements, gmap, pieces):
    rows, width = pair_elements.shape
    piece = jax.ShapeDtypeStruct((width // 2 // pieces, rows), jnp.float32)
    hbm = pl.BlockSpec(memory_space=pltpu.HBM)
    return pl.pallas_call(
        take_kernel,
        out_shape=(piece,) * pieces,
        in_specs=[pl.BlockSpec(memory_space=pltpu.SMEM), hbm, hbm],
        out_specs=(pl.BlockSpec(memory_space=pltpu.VMEM),) * pieces,
        scratch_shapes=[
            pltpu.VMEM((2, rows, width // 4), jnp.float32),
            pltpu.VMEM((rows,), jnp.int32),
            pltpu.SemaphoreType.DMA((3,)),
        ],
        cost_estimate=pl.CostEstimate(flops=3 * rows * rows * width, bytes_accessed=4 * rows * width, transcendentals=0),
        compiler_params=pltpu.CompilerParams(vmem_limit_bytes=LIMIT),
        name="take",
    )(side.reshape(1), *(pltpu.with_memory_space_constraint(x, pltpu.HBM) for x in (pair_elements, gmap)))


def solution(mesh):
    ring = chip_ring(mesh)
    n = len(ring)
    size = 2 * n
    ahead = [(a, b) for i in range(n) for a, b in zip(ring[i], ring[(i + 1) % n])]
    back = [(b, a) for a, b in ahead]
    partner = [(i, i ^ 1) for i in range(size)]
    spot_of = {index: i for i, chip in enumerate(ring) for index in chip}
    sources = [
        [[ring[(spot_of[d] - step * way) % n][0] // 2 for step in range(n)] for way in (1, -1)] for d in range(size)
    ]

    bits = [1 << i for i in range(size.bit_length() - 1)]
    phases = [tuple(reversed(bits[i : i + 2])) for i in range(0, len(bits), 2)]

    def local(pair_elements, gmap, w_screened, coulomb):
        _, width = pair_elements.shape
        half = width // 2
        wide = half // 2
        me = lax.axis_index("blk")
        core = me % 2
        source = lax.dynamic_index_in_dim(jnp.array(sources, jnp.int32), me, 0, keepdims=False)
        blocks = (2 * source.T[:, None, :] + ((core + jnp.arange(2)) % 2)[None, :, None]).reshape(n * 4)
        here = core * half
        mine = list(take(core, pair_elements, gmap, 2))
        (away,) = take(1 - core, pair_elements, gmap, 1)
        given = lax.ppermute(away, "blk", partner)
        w_late, _ = lax.optimization_barrier((w_screened, away))
        w_partner = lax.ppermute(w_late, "blk", partner)
        held = [mine, [given[way * wide : (way + 1) * wide] for way in (0, 1)]]
        start = list(held)

        band = (here + jnp.arange(half, dtype=jnp.int32)) % NB
        coef = jnp.where(band < OCC, -0.5, 0.5).astype(jnp.float32)
        start = [x for pair in start for x in pair]
        total = None
        form = None
        terms = None

        def exchange(terms, bits, left):
            at = [left.index(bit) for bit in bits]
            terms = terms.reshape((2,) * len(left) + (-1,))
            terms = jnp.moveaxis(terms, at, range(len(at))).reshape(1 << len(at), -1)
            mine = sum(((me // bit) % 2) << (len(bits) - 1 - i) for i, bit in enumerate(bits))
            kept = lax.dynamic_index_in_dim(terms, mine, 0, keepdims=False)
            for x in range(1, 1 << len(bits)):
                mask = sum(bit for i, bit in enumerate(bits) if (x >> (len(bits) - 1 - i)) & 1)
                sent = lax.dynamic_index_in_dim(terms, mine ^ x, 0, keepdims=False)
                kept = kept + lax.ppermute(sent, "blk", [(b, b ^ mask) for b in range(size)])
            return kept

        for step in range(n):
            for c in (0, 1):
                if step == n - 1 and c == 1:
                    part = wide // PARTS
                    late, others = [], []
                    for at in range(PARTS):
                        late.append(
                            [
                                lax.ppermute(x[at * part : (at + 1) * part], "blk", back if way else ahead)
                                for way, x in enumerate(held[c])
                            ]
                        )
                    terms, *late[0] = lax.optimization_barrier((terms, *late[0]))
                    for at, use in enumerate(late):
                        other = finish_partner(at, use, right, total)
                        others.append(lax.ppermute(other, "blk", partner))
                    screened = finish_own(core, [x for use in late for x in use], right, total)
                    screened = place(core, others, screened)
                    break
                if step:
                    held[c] = [lax.ppermute(held[c][way], "blk", back if way else ahead) for way in (0, 1)]
                look = c == 1 and step in (0, n // 2 - 1, n // 2)
                use = held[c]
                total, seen = dots(blocks, 4 * step + 2 * c, use, w_screened, w_partner, total, start if look else None)
                if step == n - 1:
                    right = fetch(blocks, 4 * step + 2, w_screened, w_partner)
                if look:
                    form = -seen if step == 0 else form + seen
            if step == n // 2:
                own_bare = -0.5 * jnp.sum(jnp.concatenate(mine, 0) ** 2 * coulomb[None, :], axis=1)
                away_bare = -0.5 * jnp.sum(away * away * coulomb[None, :], axis=1)
                form = own_bare + coef * jnp.sum(form, axis=1)
                terms = jnp.where(core == 0, jnp.concatenate([form, away_bare]), jnp.concatenate([away_bare, form]))
                left = [bit for phase in reversed(phases) for bit in phase]
                for phase in phases:
                    terms = exchange(terms, phase, left)
                    left = [bit for bit in left if bit not in phase]
        return screened, terms

    in_specs = (
        P(("groups", "blk"), None),
        P(("groups", "blk")),
        P("groups", "blk"),
        P(("groups", "blk")),
    )
    out_specs = (P(("groups", "blk"), None), P(("groups", "blk")))
    return jax.shard_map(local, mesh=mesh, in_specs=in_specs, out_specs=out_specs, check_vma=False)
```

```python
import functools

import jax
import jax.numpy as jnp
from jax import lax
from jax.experimental import pallas as pl
from jax.experimental.pallas import tpu as pltpu
from jax.sharding import PartitionSpec as P


NB = 64
OCC = 4
PARTS = 2
LIMIT = 20 << 20
DOTS_LIMIT = 46 << 20


def chip_ring(mesh):
    row = mesh.devices.reshape(mesh.shape["groups"], -1)[0]
    places = [tuple(getattr(d, "coords", (0, 0, i // 2))) for i, d in enumerate(row)]
    chips = {}
    for index, place in enumerate(places):
        chips.setdefault(place, []).append(index)
    ordered = []
    spread = [len({p[k] for p in chips}) for k in range(3)]
    long = max(range(3), key=lambda k: spread[k])
    lanes = {}
    for p in chips:
        lanes.setdefault(tuple(v for k, v in enumerate(p) if k != long), []).append(p)
    for number, lane in enumerate(sorted(lanes)):
        line = sorted(lanes[lane], key=lambda p: p[long])
        ordered += line[::-1] if number % 2 else line
    return [chips[p] for p in ordered]


def split(x):
    high = x.astype(jnp.bfloat16)
    return high, (x - high.astype(jnp.float32)).astype(jnp.bfloat16)


def dots_kernel(at, first, watch, ahead, blocks, x0, x1, w_own, w_partner, *refs):
    if ahead:
        fetched, fetch_sems = refs[-2:]
        refs = refs[:-2]
    left, landed, sems = refs[-3:]
    refs = refs[:-3]
    out = refs[-watch - ahead - 1]
    rows = landed.shape[1]
    wide = x0.shape[0]

    def copies(way):
        here = pl.ds(pl.multiple_of(blocks[at + way] * rows, rows), rows)
        for k, w in enumerate((w_own, w_partner)):
            yield pltpu.make_async_copy(
                w.at[here], landed.at[way, :, k * rows : (k + 1) * rows], sems.at[way, k]
            )

    for way in (0, 1):
        for copy in copies(way):
            copy.start()
    later = []
    if ahead:
        for k, w in enumerate((w_partner, w_own)):
            for way in (0, 1):
                here = pl.ds(pl.multiple_of(blocks[at + 2 + way] * rows, rows), rows)
                later.append(pltpu.make_async_copy(w.at[here], fetched.at[2 * k + way], fetch_sems.at[2 * k + way]))
    for copy in later:
        copy.start()
    for way, x in enumerate((x0, x1)):
        xh, xl = split(x[...])
        for i, part in enumerate((xh, xl, xh)):
            left[way, :, i * rows : (i + 1) * rows] = part

    def product(way):
        for copy in copies(way):
            copy.wait()
        wh, wl = split(landed[way])
        total = jnp.dot(left[way], jnp.concatenate([wh, wh, wl], 0), preferred_element_type=jnp.float32)
        mine = pl.ds(way * wide if isinstance(way, int) else pl.multiple_of(way * wide, wide), wide)
        if not first:
            total = refs[0][mine, :] + total
        out[mine, :] = total
        return total

    if watch:
        for way in (0, 1):
            seen = product(way) * jnp.concatenate([refs[1 + way][...], refs[3 + way][...]], 1)
            seen = functools.reduce(lambda p, q: p + q, [seen[:, i : i + 128] for i in range(0, 2 * rows, 128)])
            refs[-1][way * wide : (way + 1) * wide, :] = seen
    else:

        @pl.loop(0, 2)
        def _(way):
            product(way)

    for i, copy in enumerate(later):
        copy.wait()
        refs[-1][i] = jnp.concatenate(split(fetched[i]), 0)


def dots(blocks, at, pieces, w_own, w_partner, total=None, start=None, ahead=False):
    wide, rows = pieces[0].shape
    vmem = pl.BlockSpec(memory_space=pltpu.VMEM)
    hbm = pl.BlockSpec(memory_space=pltpu.HBM)
    more = [] if total is None else [total]
    watch = [] if start is None else list(start)
    shape = jax.ShapeDtypeStruct((2 * wide, 2 * rows), jnp.float32)
    form = jax.ShapeDtypeStruct((2 * wide, 128), jnp.float32)
    right = jax.ShapeDtypeStruct((4, 2 * rows, rows), jnp.bfloat16)
    more_scratch = [pltpu.VMEM((4, rows, rows), jnp.float32), pltpu.SemaphoreType.DMA((4,))] if ahead else []
    out = pl.pallas_call(
        functools.partial(dots_kernel, at, total is None, int(start is not None), int(ahead)),
        out_shape=(shape, right) if ahead else (shape, form) if watch else (shape,),
        in_specs=[pl.BlockSpec(memory_space=pltpu.SMEM), vmem, vmem, hbm, hbm] + [vmem] * (len(more) + len(watch)),
        out_specs=(vmem, vmem)[: 2 if watch or ahead else 1],
        scratch_shapes=[
            pltpu.VMEM((2, wide, 3 * rows), jnp.bfloat16),
            pltpu.VMEM((2, rows, 2 * rows), jnp.float32),
            pltpu.SemaphoreType.DMA((2, 2)),
            *more_scratch,
        ],
        input_output_aliases={5: 0} if more else {},
        cost_estimate=pl.CostEstimate(
            flops=24 * rows * rows * wide, bytes_accessed=16 * rows * rows, transcendentals=0
        ),
        compiler_params=pltpu.CompilerParams(vmem_limit_bytes=DOTS_LIMIT),
        name="dots",
    )(blocks, *pieces, w_own, w_partner, *more, *watch)
    return out if watch or ahead else (out[0], None)


def last_part(k, at, way, x, right, total):
    wide, rows = x.shape
    xh, xl = split(x[...])
    block = 2 * (1 - k) + way
    high, low = right[block, :rows], right[block, rows:]
    part = jnp.dot(
        jnp.concatenate([xh, xl, xh], 1), jnp.concatenate([high, high, low], 0), preferred_element_type=jnp.float32
    )
    top = way * total.shape[0] // 2 + at * wide
    return total[top : top + wide, k * rows : (k + 1) * rows] + part


def partner_kernel(at, x0, x1, right, total, out):
    wide = x0.shape[0]
    for way, x in enumerate((x0, x1)):
        out[way * wide : (way + 1) * wide, :] = last_part(1, at, way, x, right, total)


def finish_partner(at, pieces, right, total):
    wide, rows = pieces[0].shape
    vmem = pl.BlockSpec(memory_space=pltpu.VMEM)
    return pl.pallas_call(
        functools.partial(partner_kernel, at),
        out_shape=jax.ShapeDtypeStruct((2 * wide, rows), jnp.float32),
        in_specs=[vmem] * 4,
        out_specs=vmem,
        cost_estimate=pl.CostEstimate(flops=12 * rows * rows * wide, bytes_accessed=16 * rows * rows, transcendentals=0),
        compiler_params=pltpu.CompilerParams(vmem_limit_bytes=DOTS_LIMIT),
        name="finish",
    )(*pieces, right, total)


def send_out(value, half, way, at, turned, sems, out):
    wide = value.shape[0]
    turned[way, at] = value.T
    quarter = out.shape[1] // 4
    columns = pl.ds(pl.multiple_of((2 * half + way) * quarter + at * wide, wide), wide)
    copy = pltpu.make_async_copy(turned.at[way, at], out.at[:, columns], sems.at[way, at])
    copy.start()
    return copy


def own_kernel(core, *refs):
    late, right, total, out, turned, sems = refs[:-5], *refs[-5:]
    copies = [
        send_out(last_part(0, i // 2, i % 2, x, right, total), core[0], i % 2, i // 2, turned, sems, out)
        for i, x in enumerate(late)
    ]
    for copy in copies:
        copy.wait()


def finish_own(core, late, right, total):
    wide, rows = late[0].shape
    vmem = pl.BlockSpec(memory_space=pltpu.VMEM)
    return pl.pallas_call(
        own_kernel,
        out_shape=jax.ShapeDtypeStruct((rows, 2 * total.shape[0]), jnp.float32),
        in_specs=[pl.BlockSpec(memory_space=pltpu.SMEM)] + [vmem] * (len(late) + 2),
        out_specs=pl.BlockSpec(memory_space=pl.ANY),
        scratch_shapes=[pltpu.VMEM((2, PARTS, rows, wide), jnp.float32), pltpu.SemaphoreType.DMA((2, PARTS))],
        cost_estimate=pl.CostEstimate(flops=24 * rows * rows * wide, bytes_accessed=16 * rows * rows, transcendentals=0),
        compiler_params=pltpu.CompilerParams(vmem_limit_bytes=DOTS_LIMIT),
        name="finish_own",
    )(core.reshape(1), *late, right, total)


def place_kernel(core, *refs):
    others, out, turned, sems = refs[:PARTS], *refs[-3:]
    wide = turned.shape[3]
    copies = [
        send_out(x[way * wide : (way + 1) * wide, :], 1 - core[0], way, at, turned, sems, out)
        for at, x in enumerate(others)
        for way in (0, 1)
    ]
    for copy in copies:
        copy.wait()


def place(core, others, out):
    both, rows = others[0].shape
    return pl.pallas_call(
        place_kernel,
        out_shape=jax.ShapeDtypeStruct(out.shape, jnp.float32),
        in_specs=[pl.BlockSpec(memory_space=pltpu.SMEM)]
        + [pl.BlockSpec(memory_space=pltpu.VMEM)] * PARTS
        + [pl.BlockSpec(memory_space=pl.ANY)],
        out_specs=pl.BlockSpec(memory_space=pl.ANY),
        scratch_shapes=[pltpu.VMEM((2, PARTS, rows, both // 2), jnp.float32), pltpu.SemaphoreType.DMA((2, PARTS))],
        input_output_aliases={1 + PARTS: 0},
        compiler_params=pltpu.CompilerParams(vmem_limit_bytes=DOTS_LIMIT),
        name="place",
    )(core.reshape(1), *others, out)


def take_kernel(side, block, gmap, *refs):
    outs, landed, order, sems = refs[:-3], refs[-3], refs[-2], refs[-1]
    rows, width = block.shape
    quarter = width // 4
    copies = []
    for at in (0, 1):
        columns = pl.ds(pl.multiple_of((2 * side[0] + at) * quarter, quarter), quarter)
        copies.append(pltpu.make_async_copy(block.at[:, columns], landed.at[at], sems.at[at]))
    ordered = pltpu.make_async_copy(gmap, order, sems.at[2])
    for copy in (copies[0], ordered, copies[1]):
        copy.start()
    for copy in (*copies, ordered):
        copy.wait()
    pick = (lax.broadcasted_iota(jnp.int32, (rows, rows), 0) == lax.rem(order[...], rows)[None, :]).astype(jnp.bfloat16)
    pick = jnp.concatenate([pick, pick, pick], 0)
    for at in (0, 1):
        x = landed[at].T
        high, rest = split(x)
        rest = x - high.astype(jnp.float32)
        mid, low = split(rest)
        got = jnp.dot(jnp.concatenate([high, mid, low], 1), pick, preferred_element_type=jnp.float32)
        if len(outs) == 2:
            outs[at][...] = got
        else:
            outs[0][at * quarter : (at + 1) * quarter, :] = got


def take(side, pair_elements, gmap, pieces):
    rows, width = pair_elements.shape
    piece = jax.ShapeDtypeStruct((width // 2 // pieces, rows), jnp.float32)
    hbm = pl.BlockSpec(memory_space=pltpu.HBM)
    return pl.pallas_call(
        take_kernel,
        out_shape=(piece,) * pieces,
        in_specs=[pl.BlockSpec(memory_space=pltpu.SMEM), hbm, hbm],
        out_specs=(pl.BlockSpec(memory_space=pltpu.VMEM),) * pieces,
        scratch_shapes=[
            pltpu.VMEM((2, rows, width // 4), jnp.float32),
            pltpu.VMEM((rows,), jnp.int32),
            pltpu.SemaphoreType.DMA((3,)),
        ],
        cost_estimate=pl.CostEstimate(flops=3 * rows * rows * width, bytes_accessed=4 * rows * width, transcendentals=0),
        compiler_params=pltpu.CompilerParams(vmem_limit_bytes=LIMIT),
        name="take",
    )(side.reshape(1), *(pltpu.with_memory_space_constraint(x, pltpu.HBM) for x in (pair_elements, gmap)))


def solution(mesh):
    ring = chip_ring(mesh)
    n = len(ring)
    size = 2 * n
    ahead = [(a, b) for i in range(n) for a, b in zip(ring[i], ring[(i + 1) % n])]
    back = [(b, a) for a, b in ahead]
    partner = [(i, i ^ 1) for i in range(size)]
    spot_of = {index: i for i, chip in enumerate(ring) for index in chip}
    sources = [
        [[ring[(spot_of[d] - step * way) % n][0] // 2 for step in range(n)] for way in (1, -1)] for d in range(size)
    ]

    bits = [1 << i for i in range(size.bit_length() - 1)]
    phases = [tuple(reversed(bits[i : i + 2])) for i in range(0, len(bits), 2)]

    def local(pair_elements, gmap, w_screened, coulomb):
        _, width = pair_elements.shape
        half = width // 2
        wide = half // 2
        me = lax.axis_index("blk")
        core = me % 2
        source = lax.dynamic_index_in_dim(jnp.array(sources, jnp.int32), me, 0, keepdims=False)
        blocks = (2 * source.T[:, None, :] + ((core + jnp.arange(2)) % 2)[None, :, None]).reshape(n * 4)
        here = core * half
        mine = list(take(core, pair_elements, gmap, 2))
        (away,) = take(1 - core, pair_elements, gmap, 1)
        given = lax.ppermute(away, "blk", partner)
        w_late, _ = lax.optimization_barrier((w_screened, away))
        w_partner = lax.ppermute(w_late, "blk", partner)
        held = [mine, [given[way * wide : (way + 1) * wide] for way in (0, 1)]]
        start = list(held)

        band = (here + jnp.arange(half, dtype=jnp.int32)) % NB
        coef = jnp.where(band < OCC, -0.5, 0.5).astype(jnp.float32)
        start = [x for pair in start for x in pair]
        total = None
        form = None
        terms = None

        def exchange(terms, bits, left):
            at = [left.index(bit) for bit in bits]
            terms = terms.reshape((2,) * len(left) + (-1,))
            terms = jnp.moveaxis(terms, at, range(len(at))).reshape(1 << len(at), -1)
            mine = sum(((me // bit) % 2) << (len(bits) - 1 - i) for i, bit in enumerate(bits))
            kept = lax.dynamic_index_in_dim(terms, mine, 0, keepdims=False)
            for x in range(1, 1 << len(bits)):
                mask = sum(bit for i, bit in enumerate(bits) if (x >> (len(bits) - 1 - i)) & 1)
                sent = lax.dynamic_index_in_dim(terms, mine ^ x, 0, keepdims=False)
                kept = kept + lax.ppermute(sent, "blk", [(b, b ^ mask) for b in range(size)])
            return kept

        for step in range(n):
            for c in (0, 1):
                if step == n - 1 and c == 1:
                    part = wide // PARTS
                    late, others = [], []
                    for at in range(PARTS):
                        late.append(
                            [
                                lax.ppermute(x[at * part : (at + 1) * part], "blk", back if way else ahead)
                                for way, x in enumerate(held[c])
                            ]
                        )
                    terms, *late[0] = lax.optimization_barrier((terms, *late[0]))
                    for at, use in enumerate(late):
                        other = finish_partner(at, use, right, total)
                        others.append(lax.ppermute(other, "blk", partner))
                    screened = finish_own(core, [x for use in late for x in use], right, total)
                    screened = place(core, others, screened)
                    break
                if step:
                    held[c] = [lax.ppermute(held[c][way], "blk", back if way else ahead) for way in (0, 1)]
                look = c == 1 and step in (0, n // 2 - 1, n // 2)
                use = held[c]
                total, seen = dots(
                    blocks, 4 * step + 2 * c, use, w_screened, w_partner, total, start if look else None, step == n - 1
                )
                if step == n - 1:
                    right = seen
                if look:
                    form = -seen if step == 0 else form + seen
            if step == n // 2:
                own_bare = -0.5 * jnp.sum(jnp.concatenate(mine, 0) ** 2 * coulomb[None, :], axis=1)
                away_bare = -0.5 * jnp.sum(away * away * coulomb[None, :], axis=1)
                form = own_bare + coef * jnp.sum(form, axis=1)
                terms = jnp.where(core == 0, jnp.concatenate([form, away_bare]), jnp.concatenate([away_bare, form]))
                left = [bit for phase in reversed(phases) for bit in phase]
                for phase in phases:
                    terms = exchange(terms, phase, left)
                    left = [bit for bit in left if bit not in phase]
        return screened, terms

    in_specs = (
        P(("groups", "blk"), None),
        P(("groups", "blk")),
        P("groups", "blk"),
        P(("groups", "blk")),
    )
    out_specs = (P(("groups", "blk"), None), P(("groups", "blk")))
    return jax.shard_map(local, mesh=mesh, in_specs=in_specs, out_specs=out_specs, check_vma=False)
```

```python
import functools

import jax
import jax.numpy as jnp
from jax import lax
from jax.experimental import pallas as pl
from jax.experimental.pallas import tpu as pltpu
from jax.sharding import PartitionSpec as P


NB = 64
OCC = 4
PARTS = 2
LIMIT = 20 << 20
DOTS_LIMIT = 46 << 20


def chip_ring(mesh):
    row = mesh.devices.reshape(mesh.shape["groups"], -1)[0]
    places = [tuple(getattr(d, "coords", (0, 0, i // 2))) for i, d in enumerate(row)]
    chips = {}
    for index, place in enumerate(places):
        chips.setdefault(place, []).append(index)
    ordered = []
    spread = [len({p[k] for p in chips}) for k in range(3)]
    long = max(range(3), key=lambda k: spread[k])
    lanes = {}
    for p in chips:
        lanes.setdefault(tuple(v for k, v in enumerate(p) if k != long), []).append(p)
    for number, lane in enumerate(sorted(lanes)):
        line = sorted(lanes[lane], key=lambda p: p[long])
        ordered += line[::-1] if number % 2 else line
    return [chips[p] for p in ordered]


def split(x):
    high = x.astype(jnp.bfloat16)
    return high, (x - high.astype(jnp.float32)).astype(jnp.bfloat16)


def dots_kernel(at, first, watch, ahead, blocks, x0, x1, w_own, w_partner, *refs):
    if ahead:
        fetched, fetch_sems = refs[-2:]
        refs = refs[:-2]
    left, landed, sems = refs[-3:]
    refs = refs[:-3]
    out = refs[-watch - ahead - 1]
    rows = landed.shape[1]
    wide = x0.shape[0]

    def copies(way):
        here = pl.ds(pl.multiple_of(blocks[at + way] * rows, rows), rows)
        for k, w in enumerate((w_own, w_partner)):
            yield pltpu.make_async_copy(
                w.at[here], landed.at[way, :, k * rows : (k + 1) * rows], sems.at[way, k]
            )

    for way in (0, 1):
        for copy in copies(way):
            copy.start()
    later = []
    if ahead:
        for k, w in enumerate((w_partner, w_own)):
            for way in (0, 1):
                here = pl.ds(pl.multiple_of(blocks[at + 2 + way] * rows, rows), rows)
                later.append(pltpu.make_async_copy(w.at[here], fetched.at[2 * k + way], fetch_sems.at[2 * k + way]))
    for copy in later:
        copy.start()
    for way, x in enumerate((x0, x1)):
        xh, xl = split(x[...])
        for i, part in enumerate((xh, xl, xh)):
            left[way, :, i * rows : (i + 1) * rows] = part

    def product(way):
        for copy in copies(way):
            copy.wait()
        wh, wl = split(landed[way])
        total = jnp.dot(left[way], jnp.concatenate([wh, wh, wl], 0), preferred_element_type=jnp.float32)
        mine = pl.ds(way * wide if isinstance(way, int) else pl.multiple_of(way * wide, wide), wide)
        if not first:
            total = refs[0][mine, :] + total
        out[mine, :] = total
        return total

    if watch:
        for way in (0, 1):
            seen = product(way) * jnp.concatenate([refs[1 + way][...], refs[3 + way][...]], 1)
            seen = functools.reduce(lambda p, q: p + q, [seen[:, i : i + 128] for i in range(0, 2 * rows, 128)])
            refs[-1][way * wide : (way + 1) * wide, :] = seen
    else:

        @pl.loop(0, 2)
        def _(way):
            product(way)

    for i, copy in enumerate(later):
        copy.wait()
        refs[-1][i] = jnp.concatenate(split(fetched[i]), 0)


def dots(blocks, at, pieces, w_own, w_partner, total=None, start=None, ahead=False):
    wide, rows = pieces[0].shape
    vmem = pl.BlockSpec(memory_space=pltpu.VMEM)
    hbm = pl.BlockSpec(memory_space=pltpu.HBM)
    more = [] if total is None else [total]
    watch = [] if start is None else list(start)
    shape = jax.ShapeDtypeStruct((2 * wide, 2 * rows), jnp.float32)
    form = jax.ShapeDtypeStruct((2 * wide, 128), jnp.float32)
    right = jax.ShapeDtypeStruct((4, 2 * rows, rows), jnp.bfloat16)
    more_scratch = [pltpu.VMEM((4, rows, rows), jnp.float32), pltpu.SemaphoreType.DMA((4,))] if ahead else []
    out = pl.pallas_call(
        functools.partial(dots_kernel, at, total is None, int(start is not None), int(ahead)),
        out_shape=(shape, right) if ahead else (shape, form) if watch else (shape,),
        in_specs=[pl.BlockSpec(memory_space=pltpu.SMEM), vmem, vmem, hbm, hbm] + [vmem] * (len(more) + len(watch)),
        out_specs=(vmem, vmem)[: 2 if watch or ahead else 1],
        scratch_shapes=[
            pltpu.VMEM((2, wide, 3 * rows), jnp.bfloat16),
            pltpu.VMEM((2, rows, 2 * rows), jnp.float32),
            pltpu.SemaphoreType.DMA((2, 2)),
            *more_scratch,
        ],
        input_output_aliases={5: 0} if more else {},
        cost_estimate=pl.CostEstimate(
            flops=24 * rows * rows * wide, bytes_accessed=16 * rows * rows, transcendentals=0
        ),
        compiler_params=pltpu.CompilerParams(vmem_limit_bytes=DOTS_LIMIT),
        name="dots",
    )(blocks, *pieces, w_own, w_partner, *more, *watch)
    return out if watch or ahead else (out[0], None)


def last_part(k, at, way, x, right, total):
    wide, rows = x.shape
    xh, xl = split(x[...])
    block = 2 * (1 - k) + way
    high, low = right[block, :rows], right[block, rows:]
    part = jnp.dot(
        jnp.concatenate([xh, xl, xh], 1), jnp.concatenate([high, high, low], 0), preferred_element_type=jnp.float32
    )
    top = way * total.shape[0] // 2 + at * wide
    return total[top : top + wide, k * rows : (k + 1) * rows] + part


def partner_kernel(at, x0, x1, right, total, out):
    wide = x0.shape[0]
    for way, x in enumerate((x0, x1)):
        out[way * wide : (way + 1) * wide, :] = last_part(1, at, way, x, right, total)


def finish_partner(at, pieces, right, total):
    wide, rows = pieces[0].shape
    vmem = pl.BlockSpec(memory_space=pltpu.VMEM)
    return pl.pallas_call(
        functools.partial(partner_kernel, at),
        out_shape=jax.ShapeDtypeStruct((2 * wide, rows), jnp.float32),
        in_specs=[vmem] * 4,
        out_specs=vmem,
        cost_estimate=pl.CostEstimate(flops=12 * rows * rows * wide, bytes_accessed=16 * rows * rows, transcendentals=0),
        compiler_params=pltpu.CompilerParams(vmem_limit_bytes=DOTS_LIMIT),
        name="finish",
    )(*pieces, right, total)


def send_out(value, half, way, at, kind, turned, sems, out):
    wide = value.shape[0]
    turned[kind, way, at] = value.T
    quarter = out.shape[1] // 4
    columns = pl.ds(pl.multiple_of((2 * half + way) * quarter + at * wide, wide), wide)
    copy = pltpu.make_async_copy(turned.at[kind, way, at], out.at[:, columns], sems.at[kind, way, at])
    copy.start()
    return copy


def settle_kernel(owns, others, aliased, core, *refs):
    out, turned, sems = refs[-3:]
    refs = refs[: len(refs) - 3 - aliased]
    copies = []
    if owns:
        right, total = refs[2 * len(owns)], refs[2 * len(owns) + 1]
        for i, at in enumerate(owns):
            for way in (0, 1):
                part = last_part(0, at, way, refs[2 * i + way], right, total)
                copies.append(send_out(part, core[0], way, at, 0, turned, sems, out))
    refs = refs[len(refs) - len(others) :]
    for i, at in enumerate(others):
        wide = turned.shape[4]
        for way in (0, 1):
            part = refs[i][way * wide : (way + 1) * wide, :]
            copies.append(send_out(part, 1 - core[0], way, at, 1, turned, sems, out))
    for copy in copies:
        copy.wait()


def settle(core, owns, others, right, total, out=None):
    rows = total.shape[1] // 2
    wide = total.shape[0] // 2 // PARTS
    vmem = pl.BlockSpec(memory_space=pltpu.VMEM)
    args = [x for pair in owns.values() for x in pair] + ([right, total] if owns else []) + list(others.values())
    more = [] if out is None else [out]
    return pl.pallas_call(
        functools.partial(settle_kernel, tuple(owns), tuple(others), len(more)),
        out_shape=jax.ShapeDtypeStruct((rows, 2 * total.shape[0]), jnp.float32),
        in_specs=[pl.BlockSpec(memory_space=pltpu.SMEM)]
        + [vmem] * len(args)
        + [pl.BlockSpec(memory_space=pl.ANY)] * len(more),
        out_specs=pl.BlockSpec(memory_space=pl.ANY),
        scratch_shapes=[pltpu.VMEM((2, 2, PARTS, rows, wide), jnp.float32), pltpu.SemaphoreType.DMA((2, 2, PARTS))],
        input_output_aliases={1 + len(args): 0} if more else {},
        cost_estimate=pl.CostEstimate(flops=24 * rows * rows * wide, bytes_accessed=16 * rows * rows, transcendentals=0),
        compiler_params=pltpu.CompilerParams(vmem_limit_bytes=DOTS_LIMIT),
        name="settle",
    )(core.reshape(1), *args, *more)


def take_kernel(side, block, gmap, *refs):
    outs, landed, order, sems = refs[:-3], refs[-3], refs[-2], refs[-1]
    rows, width = block.shape
    quarter = width // 4
    copies = []
    for at in (0, 1):
        columns = pl.ds(pl.multiple_of((2 * side[0] + at) * quarter, quarter), quarter)
        copies.append(pltpu.make_async_copy(block.at[:, columns], landed.at[at], sems.at[at]))
    ordered = pltpu.make_async_copy(gmap, order, sems.at[2])
    for copy in (copies[0], ordered, copies[1]):
        copy.start()
    for copy in (*copies, ordered):
        copy.wait()
    pick = (lax.broadcasted_iota(jnp.int32, (rows, rows), 0) == lax.rem(order[...], rows)[None, :]).astype(jnp.bfloat16)
    pick = jnp.concatenate([pick, pick, pick], 0)
    for at in (0, 1):
        x = landed[at].T
        high, rest = split(x)
        rest = x - high.astype(jnp.float32)
        mid, low = split(rest)
        got = jnp.dot(jnp.concatenate([high, mid, low], 1), pick, preferred_element_type=jnp.float32)
        if len(outs) == 2:
            outs[at][...] = got
        else:
            outs[0][at * quarter : (at + 1) * quarter, :] = got


def take(side, pair_elements, gmap, pieces):
    rows, width = pair_elements.shape
    piece = jax.ShapeDtypeStruct((width // 2 // pieces, rows), jnp.float32)
    hbm = pl.BlockSpec(memory_space=pltpu.HBM)
    return pl.pallas_call(
        take_kernel,
        out_shape=(piece,) * pieces,
        in_specs=[pl.BlockSpec(memory_space=pltpu.SMEM), hbm, hbm],
        out_specs=(pl.BlockSpec(memory_space=pltpu.VMEM),) * pieces,
        scratch_shapes=[
            pltpu.VMEM((2, rows, width // 4), jnp.float32),
            pltpu.VMEM((rows,), jnp.int32),
            pltpu.SemaphoreType.DMA((3,)),
        ],
        cost_estimate=pl.CostEstimate(flops=3 * rows * rows * width, bytes_accessed=4 * rows * width, transcendentals=0),
        compiler_params=pltpu.CompilerParams(vmem_limit_bytes=LIMIT),
        name="take",
    )(side.reshape(1), *(pltpu.with_memory_space_constraint(x, pltpu.HBM) for x in (pair_elements, gmap)))


def solution(mesh):
    ring = chip_ring(mesh)
    n = len(ring)
    size = 2 * n
    ahead = [(a, b) for i in range(n) for a, b in zip(ring[i], ring[(i + 1) % n])]
    back = [(b, a) for a, b in ahead]
    partner = [(i, i ^ 1) for i in range(size)]
    spot_of = {index: i for i, chip in enumerate(ring) for index in chip}
    sources = [
        [[ring[(spot_of[d] - step * way) % n][0] // 2 for step in range(n)] for way in (1, -1)] for d in range(size)
    ]

    bits = [1 << i for i in range(size.bit_length() - 1)]
    phases = [tuple(reversed(bits[i : i + 2])) for i in range(0, len(bits), 2)]

    def local(pair_elements, gmap, w_screened, coulomb):
        _, width = pair_elements.shape
        half = width // 2
        wide = half // 2
        me = lax.axis_index("blk")
        core = me % 2
        source = lax.dynamic_index_in_dim(jnp.array(sources, jnp.int32), me, 0, keepdims=False)
        blocks = (2 * source.T[:, None, :] + ((core + jnp.arange(2)) % 2)[None, :, None]).reshape(n * 4)
        here = core * half
        mine = list(take(core, pair_elements, gmap, 2))
        (away,) = take(1 - core, pair_elements, gmap, 1)
        given = lax.ppermute(away, "blk", partner)
        w_late, _ = lax.optimization_barrier((w_screened, away))
        w_partner = lax.ppermute(w_late, "blk", partner)
        held = [mine, [given[way * wide : (way + 1) * wide] for way in (0, 1)]]
        start = list(held)

        band = (here + jnp.arange(half, dtype=jnp.int32)) % NB
        coef = jnp.where(band < OCC, -0.5, 0.5).astype(jnp.float32)
        start = [x for pair in start for x in pair]
        total = None
        form = None
        terms = None

        def exchange(terms, bits, left):
            at = [left.index(bit) for bit in bits]
            terms = terms.reshape((2,) * len(left) + (-1,))
            terms = jnp.moveaxis(terms, at, range(len(at))).reshape(1 << len(at), -1)
            mine = sum(((me // bit) % 2) << (len(bits) - 1 - i) for i, bit in enumerate(bits))
            kept = lax.dynamic_index_in_dim(terms, mine, 0, keepdims=False)
            for x in range(1, 1 << len(bits)):
                mask = sum(bit for i, bit in enumerate(bits) if (x >> (len(bits) - 1 - i)) & 1)
                sent = lax.dynamic_index_in_dim(terms, mine ^ x, 0, keepdims=False)
                kept = kept + lax.ppermute(sent, "blk", [(b, b ^ mask) for b in range(size)])
            return kept

        for step in range(n):
            for c in (0, 1):
                if step == n - 1 and c == 1:
                    part = wide // PARTS
                    late, others = [], []
                    for at in range(PARTS):
                        late.append(
                            [
                                lax.ppermute(x[at * part : (at + 1) * part], "blk", back if way else ahead)
                                for way, x in enumerate(held[c])
                            ]
                        )
                    terms, *late[0] = lax.optimization_barrier((terms, *late[0]))
                    screened = None
                    for at, use in enumerate(late):
                        other = finish_partner(at, use, right, total)
                        others.append(lax.ppermute(other, "blk", partner))
                        done = {at - 1: others[at - 1]} if at else {}
                        screened = settle(core, {at: use}, done, right, total, screened)
                    screened = settle(core, {}, {PARTS - 1: others[-1]}, right, total, screened)
                    break
                if step:
                    held[c] = [lax.ppermute(held[c][way], "blk", back if way else ahead) for way in (0, 1)]
                look = c == 1 and step in (0, n // 2 - 1, n // 2)
                use = held[c]
                total, seen = dots(
                    blocks, 4 * step + 2 * c, use, w_screened, w_partner, total, start if look else None, step == n - 1
                )
                if step == n - 1:
                    right = seen
                if look:
                    form = -seen if step == 0 else form + seen
            if step == n // 2:
                own_bare = -0.5 * jnp.sum(jnp.concatenate(mine, 0) ** 2 * coulomb[None, :], axis=1)
                away_bare = -0.5 * jnp.sum(away * away * coulomb[None, :], axis=1)
                form = own_bare + coef * jnp.sum(form, axis=1)
                terms = jnp.where(core == 0, jnp.concatenate([form, away_bare]), jnp.concatenate([away_bare, form]))
                left = [bit for phase in reversed(phases) for bit in phase]
                for phase in phases:
                    terms = exchange(terms, phase, left)
                    left = [bit for bit in left if bit not in phase]
        return screened, terms

    in_specs = (
        P(("groups", "blk"), None),
        P(("groups", "blk")),
        P("groups", "blk"),
        P(("groups", "blk")),
    )
    out_specs = (P(("groups", "blk"), None), P(("groups", "blk")))
    return jax.shard_map(local, mesh=mesh, in_specs=in_specs, out_specs=out_specs, check_vma=False)
```
